256 devices in a mesh: dp: 16 (over x, z_lo), space: 8 (over y, core), chan: 2 (over z_hi).
Axes of the slice: x: 4, y: 4, z: 8 (z_hi: 2, z_lo: 4; z = z_hi * 4 + z_lo), core: 2. Of those that a mesh axis runs over, the one named last changes fastest.
Arguments:
- pixels: bfloat16 [16, 64, 64, 512], P('dp', 'space'), may hold values from -6 to 6
- hidden: bfloat16 [16, 128, 4096], P('dp', None, 'space'), may hold values from -6 to 6
- enc_gain: bfloat16 [4096], replicated, may hold values from 0.099609375 to 1.8984375
- lengths: int32 [16], P('dp'), may hold values from 1 to 128
- time_steps: int32 [16], P('dp'), may hold values from 0 to 999
- attn_gain: bfloat16 [512], replicated, may hold values from 0.099609375 to 1.8984375
- w_query: bfloat16 [512, 512], P(None, 'chan'), may hold values from -1 to 1
- w_key: bfloat16 [4096, 512], P(None, 'chan'), may hold values from -1 to 1
- w_value: bfloat16 [4096, 512], P(None, 'chan'), may hold values from -0.09375 to 0.09375
- w_out: bfloat16 [512, 512], P('chan'), may hold values from -0.25 to 0.25
- w_time: bfloat16 [512, 1024], replicated, may hold values from -0.25 to 0.25
- w_conv: bfloat16 [4608, 512], P(None, 'chan'), may hold values from -0.09375 to 0.09375
- cotangent: bfloat16 [16, 64, 64, 512], P('dp', 'space', None, 'chan'), may hold values from -6 to 6
Outputs:
- result: bfloat16 [16, 64, 64, 512], P('dp', 'space', None, 'chan')
- grad_conv: float32 [4608, 512], P(('dp', 'space'), 'chan')
- grad_out_t: float32 [512, 512], P(('dp', 'space'), 'chan')
The draws below stay inside these ranges and needn't reach their ends.
All inputs are finite; a program needn't handle non-finite values.
Results may differ from the reference program's by a relative error of at most 0.01.
The reference program's roundings to bfloat16 on the way (of `context`, `key_proj`, `query_proj`, `weights_soft`, `attended`, `activation` and `grad_mixed`) count: a program that leaves them out, or rounds other values in their place, can miss the bound.
Values may be sent and summed in bfloat16 or wider, within the bound.
A program may use at most 128 MiB of HBM per device.

```python
import math
import jax
import jax.numpy as jnp
from jax import lax

ENC = 4096
HEADS = 8
HEAD_DIM = 64
TEMB = 512
CAP_LEN = 128
COLS = 64
CH = 512
IMAGES = 16
HEIGHT = 64


def drawn_weight(key, salt, rows, cols):
    noise_key = jax.random.fold_in(key, salt)
    values = jax.random.truncated_normal(noise_key, -4.0, 4.0, (rows, cols), jnp.float32) * rows ** (-0.5)
    return values.astype(jnp.bfloat16)


def draw_w_query(key, part):
    return drawn_weight(key, 17, CH, CH)


def draw_w_key(key, part):
    return drawn_weight(key, 23, ENC, CH)


def plant(values, stream_key, least, high):
    spot = [jax.random.randint(jax.random.fold_in(stream_key, axis), (), 0, length) for axis, length in enumerate(values.shape)]
    widest = values.shape.index(max(values.shape))
    beside = spot[:widest] + [(spot[widest] + 1) % values.shape[widest]] + spot[widest + 1:]
    return values.at[tuple(spot)].set(least).at[tuple(beside)].set(high)


def level_of(own_key, shape, shards, least, largest):
    factor_of = 1.0
    for axis_at, blocks in shards:
        draws = jax.random.uniform(jax.random.fold_in(jax.random.fold_in(own_key, 6), axis_at), (blocks,), jnp.float32, least / len(shards), largest / len(shards))
        factor_of = factor_of * jnp.repeat(jnp.exp(draws), shape[axis_at] // blocks).reshape((-1,) + (1,) * (len(shape) - 1 - axis_at))
    return factor_of


def bell_draw(stream_key, extent, spread, limit, shards=(), kind=jnp.bfloat16):
    gain = level_of(stream_key, extent, shards, -0.22, 0.18) if shards else 1.0
    entries = jax.random.normal(stream_key, extent, jnp.float32) * spread * gain
    return jnp.minimum(jnp.maximum(entries, -limit), limit).astype(kind)


def setup_inputs(seed: int = 0) -> dict:
    streams_of = jax.random.split(jax.random.key(seed), 14)
    pixels = bell_draw(streams_of[0], (IMAGES, HEIGHT, COLS, CH), 1.0, 6.0, ((0, 16), (1, 8)))
    hidden = bell_draw(streams_of[1], (IMAGES, CAP_LEN, ENC), 1.0, 6.0, ((0, 16), (2, 8)))
    enc_gain = jnp.clip(1.0 + 0.18 * jax.random.normal(streams_of[2], (ENC,), jnp.float32), 0.099609375, 1.8984375).astype(jnp.bfloat16)
    lengths = plant(jax.random.randint(streams_of[3], (IMAGES,), 1, CAP_LEN + 1), jax.random.fold_in(streams_of[3], 1), 1, CAP_LEN).astype(jnp.int32)
    time_steps = plant(jax.random.randint(streams_of[4], (IMAGES,), 0, 1000), jax.random.fold_in(streams_of[4], 1), 0, 999).astype(jnp.int32)
    attn_gain = jnp.clip(1.0 + 0.18 * jax.random.normal(streams_of[5], (CH,), jnp.float32), 0.099609375, 1.8984375).astype(jnp.bfloat16)
    w_query = draw_w_query(jax.random.fold_in(streams_of[13], 71), 0)
    w_key = draw_w_key(jax.random.fold_in(streams_of[13], 71), 0)
    w_value = bell_draw(streams_of[8], (ENC, CH), ENC ** -0.5, 0.09375, ((1, 2),))
    w_out = bell_draw(streams_of[9], (CH, CH), CH ** -0.5, 0.25, ((0, 2),))
    w_time = bell_draw(streams_of[10], (TEMB, 2 * CH), TEMB ** -0.5, 0.25)
    w_conv = bell_draw(streams_of[11], (9 * CH, CH), (9 * CH) ** -0.5, 0.09375, ((1, 2),))
    cotangent = bell_draw(streams_of[12], (IMAGES, HEIGHT, COLS, CH), 1.0, 6.0, ((0, 16), (1, 8), (3, 2)))
    return {"pixels": pixels, "hidden": hidden, "enc_gain": enc_gain, "lengths": lengths, "time_steps": time_steps, "attn_gain": attn_gain, "w_query": w_query, "w_key": w_key, "w_value": w_value, "w_out": w_out, "w_time": w_time, "w_conv": w_conv, "cotangent": cotangent}


def rms_scale(source, gain_row):
    source_f = source.astype(jnp.float32)
    mean_sq = lax.optimization_barrier(jnp.mean(source_f * source_f, axis=-1, keepdims=True))
    return source_f * lax.rsqrt(mean_sq + 1e-06) * gain_row.astype(jnp.float32)

def time_embed(time_steps, emb_width):
    half_width = emb_width // 2
    frequency = jnp.exp(-math.log(10000.0) * jnp.arange(half_width).astype(jnp.float32) / half_width)
    angles = time_steps.astype(jnp.float32)[:, None] * frequency[None, :]
    return jnp.concatenate([jnp.sin(angles), jnp.cos(angles)], axis=1).astype(jnp.bfloat16)

def tap_stack(padded, row_count, col_count, flipped):
    tap_parts = []
    for tap_row in range(3):
        for tap_col in range(3):
            start_row = 2 - tap_row if flipped else tap_row
            start_col = 2 - tap_col if flipped else tap_col
            tap_parts.append(padded[:, start_row:start_row + row_count, start_col:start_col + col_count, :])
    return jnp.concatenate(tap_parts, axis=-1)

def reference(pixels, hidden, enc_gain, lengths, time_steps, attn_gain, w_query, w_key, w_value, w_out, w_time, w_conv, cotangent):
    full_width = HEADS * HEAD_DIM
    context = rms_scale(hidden, enc_gain).astype(jnp.bfloat16).astype(jnp.float32)
    key_proj = jnp.einsum('cle,ef->clf', context, w_key.astype(jnp.float32)).astype(jnp.bfloat16)
    value_proj = jnp.einsum('cle,ef->clf', context, w_value.astype(jnp.float32)).astype(jnp.bfloat16)
    film_out = jnp.dot(time_embed(time_steps, TEMB), w_time, preferred_element_type=jnp.float32)
    w_back = w_conv.reshape(9, full_width, full_width).transpose(0, 2, 1).reshape(9 * full_width, full_width)

    def one_image(totals, items):
        one_pixels, key_img, value_img, cap_length, film_row, cot_image = items
        flat_pix = one_pixels.reshape(-1, full_width)
        normed = rms_scale(flat_pix, attn_gain).astype(jnp.bfloat16)
        query_proj = jnp.dot(normed, w_query, preferred_element_type=jnp.float32).astype(jnp.bfloat16)
        query_heads = query_proj.reshape(-1, HEADS, HEAD_DIM).astype(jnp.float32)
        key_heads = key_img.reshape(CAP_LEN, HEADS, HEAD_DIM).astype(jnp.float32)
        value_heads = value_img.reshape(CAP_LEN, HEADS, HEAD_DIM).astype(jnp.float32)
        scores = jnp.einsum('phd,jhd->hpj', query_heads, key_heads) * HEAD_DIM ** (-0.5)
        key_live = jnp.arange(CAP_LEN) < cap_length
        scores = jnp.where(key_live[None, None, :], scores, -1e+30)
        weights_soft = jax.nn.softmax(scores, axis=-1).astype(jnp.bfloat16).astype(jnp.float32)
        attended = jnp.einsum('hpj,jhd->phd', weights_soft, value_heads).astype(jnp.bfloat16).reshape(-1, full_width)
        mixed_res = flat_pix.astype(jnp.float32) + jnp.dot(attended, w_out, preferred_element_type=jnp.float32)
        film_scale = film_row[:full_width]
        film_shift = film_row[full_width:]
        lifted = mixed_res * (1.0 + film_scale) + film_shift
        activation = jax.nn.silu(lifted).astype(jnp.bfloat16).reshape(HEIGHT, COLS, full_width)
        padded = jnp.pad(activation, ((1, 1), (1, 1), (0, 0)))[None]
        patches = tap_stack(padded, HEIGHT, COLS, False).reshape(-1, 9 * full_width)
        conv_out = jnp.dot(patches, w_conv, preferred_element_type=jnp.float32)
        result = (mixed_res + conv_out).astype(jnp.bfloat16).reshape(HEIGHT, COLS, full_width)
        cot_flat = cot_image.reshape(-1, full_width)
        cot_padded = jnp.pad(cot_image, ((1, 1), (1, 1), (0, 0)))[None]
        cot_patches = tap_stack(cot_padded, HEIGHT, COLS, True).reshape(-1, 9 * full_width)
        grad_act = jnp.dot(cot_patches, w_back, preferred_element_type=jnp.float32)
        sigmoid_u = jax.nn.sigmoid(lifted)
        grad_lift = grad_act * sigmoid_u * (1.0 + lifted * (1.0 - sigmoid_u))
        grad_mixed = (cot_flat.astype(jnp.float32) + grad_lift * (1.0 + film_scale)).astype(jnp.bfloat16)
        conv_term = lax.dot_general(patches, cot_flat, (((0,), (0,)), ((), ())), preferred_element_type=jnp.float32)
        out_term = lax.dot_general(grad_mixed, attended, (((0,), (0,)), ((), ())), preferred_element_type=jnp.float32)
        return ((totals[0] + conv_term, totals[1] + out_term), result)
    start_totals = (jnp.zeros((9 * full_width, full_width), jnp.float32), jnp.zeros((full_width, full_width), jnp.float32))
    sums, result = lax.scan(one_image, start_totals, (pixels, key_proj, value_proj, lengths, film_out, cotangent))
    return (result, sums[0], sums[1])
```

```python
import math

import jax
import jax.numpy as jnp
from jax import lax
from jax.experimental import pallas as pl
from jax.experimental.pallas import tpu as pltpu
from jax.sharding import Mesh
from jax.sharding import PartitionSpec as P

TEMB = 512
SPACE = ("space_0", "space_1")
DP_SPACE = ("dp_0", "dp_1", "space_0", "space_1")
DP = ("dp_0", "dp_1")
F32 = jnp.float32
BF16 = jnp.bfloat16
MESH = pl.DeviceIdType.MESH

ROWS = 8
COLS = 64
PIX = ROWS * COLS
EXT = PIX + 2 * COLS
CH = 512
HALF = 256
TOK = 128
PIECE = 16
STEP = 128


def dot(a, b):
    return jnp.dot(a, b, preferred_element_type=F32)


def dot_nt(a, b):
    return lax.dot_general(a, b, (((1,), (1,)), ((), ())), preferred_element_type=F32)


def dot_tn(a, b):
    return lax.dot_general(a, b, (((0,), (0,)), ((), ())), preferred_element_type=F32)


def silu_gate(lifted):
    return 1.0 / (1.0 + jnp.exp(-lifted))


def shifted_columns(wide, store):
    col = lax.rem(lax.broadcasted_iota(jnp.int32, wide.shape, 0), COLS)
    down = pltpu.roll(wide, 1, 0)
    up = pltpu.roll(wide, wide.shape[0] - 1, 0)
    store(0, jnp.where(col == 0, 0.0, down).astype(BF16))
    store(1, wide.astype(BF16))
    store(2, jnp.where(col == COLS - 1, 0.0, up).astype(BF16))


def block_rows(tap):
    pieces = []
    row = tap * CH
    while row < (tap + 1) * CH:
        block, inside = divmod(row, 72)
        count = min(72 - inside, (tap + 1) * CH - row)
        pieces.append((block, inside, row - tap * CH, count))
        row += count
    return pieces


def place_of(half, block):
    x, z, y = block // 16, (block // 4) % 4, block % 4
    return x * 16 + y * 4 + z if half == 0 else y * 16 + x * 4 + z


def kernel(
    lengths,
    pix_in,
    hid_in,
    small,
    wq_in,
    wk_in,
    wv_in,
    wo_in,
    wt_in,
    wc_in,
    cot_in,
    res_out,
    gconv_out,
    gout_out,
    pix,
    cot,
    hid,
    wq,
    wk,
    wv,
    wo,
    wt,
    wc,
    kv,
    film,
    att,
    mix,
    act3,
    cot3,
    gact_send,
    gact_recv,
    gact_own,
    result,
    cv,
    core_send,
    core_recv,
    s1,
    r1,
    a1,
    s2,
    r2,
    a2,
    s3,
    r3,
    a3,
    conv_peer,
    out_peer,
    load_sem,
    send_sem,
    recv_sem,
):
    x = lax.axis_index("dp_0")
    z = lax.axis_index("dp_1")
    y = lax.axis_index("space_0")
    core = lax.axis_index("space_1")
    chan = lax.axis_index("chan")
    other = 1 - chan
    slab = y * 2 + core
    count = [0]

    def remote(src, dst, device):
        i = count[0]
        count[0] += 1
        return pltpu.make_async_remote_copy(
            src_ref=src,
            dst_ref=dst,
            send_sem=send_sem.at[i],
            recv_sem=recv_sem.at[i],
            device_id=device,
            device_id_type=MESH,
        )

    def slab_device(d):
        s = lax.rem(slab + d, 8)
        return {"space_0": s // 2, "space_1": lax.rem(s, 2)}

    u = x * (1 - core) + y * core
    v = y * (1 - core) + x * core

    def first_device(d):
        t = lax.rem(u + d, 4)
        return {"dp_0": t * (1 - core) + x * core, "space_0": y * (1 - core) + t * core}

    def second_device(d):
        t = lax.rem(v + d, 4)
        return {"dp_0": x * (1 - core) + t * core, "space_0": t * (1 - core) + y * core}

    def depth_device(d):
        return {"dp_1": lax.rem(z + d, 4)}

    peer_chan = {"chan": other}
    peer_core = {"space_1": 1 - core}
    half_x, low_x = x // 2, lax.rem(x, 2)
    dest = [{"dp_0": 2 * chan + low_x, "space_1": k, "chan": 1 - half_x} for k in range(2)]
    source = [{"dp_0": 2 * (1 - chan) + low_x, "space_1": k, "chan": half_x} for k in range(2)]

    barrier = pltpu.get_barrier_semaphore()
    greeted = (
        [slab_device(d) for d in range(1, 8)]
        + [peer_chan]
        + [{"dp_0": lax.rem(x + d, 4)} for d in range(1, 4)]
        + [depth_device(d) for d in range(1, 4)]
        + dest
        + source
    )
    for device in greeted:
        pl.semaphore_signal(barrier, inc=1, device_id=device, device_id_type=MESH)

    loads = []

    def load(src, dst):
        copy = pltpu.make_async_copy(src, dst, load_sem.at[len(loads)])
        copy.start()
        loads.append(copy)
        return copy

    ld_cot = load(cot_in, cot.at[COLS : COLS + PIX, :])
    ld_hid = load(hid_in.at[pl.ds(slab * PIECE, PIECE), :], hid.at[slab])
    ld_wc = load(wc_in, wc)
    ld_pix = load(pix_in, pix.at[COLS : COLS + PIX, :])
    ld_wk = load(wk_in, wk)
    ld_wv = load(wv_in, wv)
    ld_wq = load(wq_in, wq.at[chan])
    ld_wo = load(wo_in, wo.at[chan])
    ld_wt = load(wt_in, wt)

    pl.semaphore_wait(barrier, len(greeted))

    hid_copies = []
    for d in range(1, 8):
        s = lax.rem(slab + d, 8)
        hid_copies.append(
            remote(hid_in.at[pl.ds(s * PIECE, PIECE), :], hid.at[slab], slab_device(d))
        )
        hid_copies[-1].start()
    halos = [
        remote(cot_in.at[PIX - COLS : PIX, :], cot.at[0:COLS, :], slab_device(1)),
        remote(cot_in.at[0:COLS, :], cot.at[COLS + PIX : EXT, :], slab_device(7)),
        remote(pix_in.at[PIX - COLS : PIX, :], pix.at[0:COLS, :], slab_device(1)),
        remote(pix_in.at[0:COLS, :], pix.at[COLS + PIX : EXT, :], slab_device(7)),
    ]
    for copy in halos:
        copy.start()
    wq_rows = pl.ds(slab * 64, 64)
    wo_rows = pl.ds(slab * 32, 32)
    w_copies = [
        remote(wq_in.at[wq_rows, :], wq.at[chan, wq_rows, :], peer_chan),
        remote(wo_in.at[wo_rows, :], wo.at[chan, wo_rows, :], peer_chan),
    ]
    for copy in w_copies:
        copy.start()

    top = (slab > 0).astype(F32)
    bottom = (slab < 7).astype(F32)

    ld_cot.wait()
    halos[0].wait()
    halos[1].wait()

    def put_cot(b, value):
        cot3[b] = value

    wide = jnp.concatenate(
        [
            cot[0:COLS, :].astype(F32) * top,
            cot[COLS : COLS + PIX, :].astype(F32),
            cot[COLS + PIX : EXT, :].astype(F32) * bottom,
        ],
        axis=0,
    )
    shifted_columns(wide, put_cot)
    ld_wc.wait()

    def grad_half(which, m):
        total = None
        for a in range(3):
            for b in range(3):
                tap = 3 * a + b
                left = cot3[2 - b, pl.ds(pl.multiple_of((2 - a) * COLS + m * STEP, COLS), STEP), :]
                rows = pl.ds(pl.multiple_of(tap * CH + which * HALF, HALF), HALF)
                term = dot_nt(left, wc[rows, :])
                total = term if total is None else total + term
        return total

    @pl.loop(0, PIX // STEP)
    def _(m):
        rows = pl.ds(pl.multiple_of(m * STEP, STEP), STEP)
        gact_send[rows, :] = grad_half(other, m).astype(BF16)

    ld_hid.wait()
    for copy in hid_copies:
        copy.wait()
    ld_wk.wait()
    ld_wv.wait()
    squares = None
    for s in range(8):
        part = hid[s].astype(F32)
        part = jnp.sum(part * part, axis=-1, keepdims=True)
        squares = part if squares is None else squares + part
    scale = lax.rsqrt(squares / 4096.0 + 1e-06)
    key_sum, value_sum = None, None
    for s in range(8):
        context = (hid[s].astype(F32) * scale * small[s : s + 1, :]).astype(BF16)
        key_part = dot(context, wk[s * CH : (s + 1) * CH, :])
        value_part = dot(context, wv[s * CH : (s + 1) * CH, :])
        key_sum = key_part if key_sum is None else key_sum + key_part
        value_sum = value_part if value_sum is None else value_sum + value_part
    own_tokens = pl.ds(pl.multiple_of(slab * PIECE, PIECE), PIECE)
    kv[chan, own_tokens, 0:HALF] = key_sum.astype(BF16)
    kv[chan, own_tokens, HALF:CH] = value_sum.astype(BF16)
    kv_cross = remote(kv.at[chan, own_tokens, :], kv.at[chan, own_tokens, :], peer_chan)
    kv_cross.start()
    kv_copies = []
    for d in range(1, 8):
        kv_copies.append(
            remote(kv.at[chan, own_tokens, :], kv.at[chan, own_tokens, :], slab_device(d))
        )
        kv_copies[-1].start()
    gact_cross = remote(gact_send, gact_recv, peer_chan)
    gact_cross.start()

    w_spread = []
    for copy in w_copies:
        copy.wait()
    for d in range(1, 8):
        w_spread.append(
            remote(wq.at[other, wq_rows, :], wq.at[other, wq_rows, :], slab_device(d))
        )
        w_spread[-1].start()
        w_spread.append(
            remote(wo.at[other, wo_rows, :], wo.at[other, wo_rows, :], slab_device(d))
        )
        w_spread[-1].start()

    @pl.loop(0, PIX // STEP)
    def _(m):
        rows = pl.ds(pl.multiple_of(m * STEP, STEP), STEP)
        gact_own[rows, :] = grad_half(chan, m)

    ld_wt.wait()
    time_row = jnp.broadcast_to(small[9:10, :], (16, CH)).astype(BF16)
    film_rows = dot(time_row, wt[...])
    for h in range(2):
        film[h, 0] = film_rows[0:8, h * HALF : (h + 1) * HALF]
        film[h, 1] = film_rows[0:8, CH + h * HALF : CH + (h + 1) * HALF]

    kv_cross.wait()
    kv_spread = []
    for d in range(1, 8):
        kv_spread.append(
            remote(kv.at[other, own_tokens, :], kv.at[other, own_tokens, :], slab_device(d))
        )
        kv_spread[-1].start()

    ld_pix.wait()
    ld_wq.wait()
    ld_wo.wait()
    halos[2].wait()
    halos[3].wait()
    for copy in kv_copies:
        copy.wait()
    lane = lax.broadcasted_iota(jnp.int32, (TOK, STEP), 1)
    low_lanes = lane < 64
    live = lax.broadcasted_iota(jnp.int32, (STEP, TOK), 1) < lengths[0]
    zero = jnp.zeros((TOK, STEP), BF16)

    def attend(group):
        @pl.loop(0, EXT // STEP)
        def _(m):
            rows = pl.ds(pl.multiple_of(m * STEP, STEP), STEP)
            part = pix[rows, :].astype(F32)
            mean = jnp.sum(part * part, axis=-1, keepdims=True) / 512.0
            normed = (part * lax.rsqrt(mean + 1e-06) * small[8:9, :]).astype(BF16)
            query = dot(normed, wq[group]).astype(BF16)
            for pair in range(2):
                at = pair * STEP
                keys = kv[group, :, at : at + STEP]
                values = kv[group, :, HALF + at : HALF + at + STEP]
                total = None
                for head in range(2):
                    keep = low_lanes if head == 0 else jnp.logical_not(low_lanes)
                    scores = dot_nt(query[:, at : at + STEP], jnp.where(keep, keys, zero)) * 0.125
                    scores = jnp.where(live, scores, -1e30)
                    peak = jnp.max(scores, axis=-1, keepdims=True)
                    raised = jnp.exp(scores - peak)
                    soft = raised / jnp.sum(raised, axis=-1, keepdims=True)
                    term = dot(soft.astype(BF16), jnp.where(keep, values, zero))
                    total = term if total is None else total + term
                att[group, rows, at : at + STEP] = total.astype(BF16)

    attend(chan)
    for copy in w_spread:
        copy.wait()
    for copy in kv_spread:
        copy.wait()
    attend(other)

    @pl.loop(0, EXT // STEP)
    def _(m):
        rows = pl.ds(pl.multiple_of(m * STEP, STEP), STEP)
        mixed = pix[rows, :].astype(F32) + dot(att[0, rows, :], wo[0]) + dot(att[1, rows, :], wo[1])
        mix[0, rows, :] = mixed[:, 0:HALF]
        mix[1, rows, :] = mixed[:, HALF:CH]

    for h in range(2):
        lifted = mix[h] * (1.0 + film[h, 0, 0:1, :]) + film[h, 1, 0:1, :]
        active = lifted * silu_gate(lifted)
        active = jnp.concatenate(
            [active[0:COLS] * top, active[COLS : COLS + PIX], active[COLS + PIX : EXT] * bottom],
            axis=0,
        )

        def put_act(b, value):
            act3[b, :, h * HALF : (h + 1) * HALF] = value

        shifted_columns(active.astype(BF16).astype(F32), put_act)

    for tap in range(9):
        a, b = divmod(tap, 3)
        term = dot_tn(act3[b, a * COLS : a * COLS + PIX, :], cot[COLS : COLS + PIX, :])
        for block, inside, row, size in block_rows(tap):
            for h in range(2):
                cv[h, place_of(h, block), inside : inside + size, :] = term[
                    row : row + size, h * STEP : (h + 1) * STEP
                ]

    gact_cross.wait()

    @pl.loop(0, PIX // STEP)
    def _(m):
        rows = pl.ds(pl.multiple_of(m * STEP, STEP), STEP)
        rows_ext = pl.ds(pl.multiple_of(m * STEP + COLS, COLS), STEP)
        gain = 1.0 + film[chan, 0, 0:1, :]
        lifted = mix[chan, rows_ext, :] * gain + film[chan, 1, 0:1, :]
        gate = silu_gate(lifted)
        grad_act = gact_own[rows, :] + gact_recv[rows, :].astype(F32)
        grad_lift = grad_act * gate * (1.0 + lifted * (1.0 - gate))
        gact_own[rows, :] = cot[rows_ext, :].astype(F32) + grad_lift * gain

    grad_mixed = gact_own[...].astype(BF16)
    for to in range(2):
        term = dot_tn(grad_mixed, att[to, COLS : COLS + PIX, :])
        for low in range(2):
            for zz in range(4):
                for yy in range(4):
                    row = low * 128 + zz * 32 + yy * 8
                    block = (2 * (1 - to) + low) * 16 + zz * 4 + yy
                    for h in range(2):
                        cv[h, place_of(h, block), 72:80, :] = term[
                            row : row + 8, h * STEP : (h + 1) * STEP
                        ]

    @pl.loop(0, 64)
    def _(i):
        core_send[i] = cv[1 - core, i].astype(BF16)

    to_core = remote(core_send, core_recv, peer_core)
    to_core.start()

    @pl.loop(0, PIX // STEP)
    def _(m):
        rows = pl.ds(pl.multiple_of(m * STEP, STEP), STEP)
        rows_ext = pl.ds(pl.multiple_of(m * STEP + COLS, COLS), STEP)
        total = mix[chan, rows_ext, :]
        for a in range(3):
            for b in range(3):
                tap = 3 * a + b
                left = act3[b, pl.ds(pl.multiple_of(a * COLS + m * STEP, COLS), STEP), :]
                total = total + dot(left, wc[tap * CH : (tap + 1) * CH, :])
        result[rows, :] = total.astype(BF16)

    put_result = pltpu.make_async_copy(result, res_out, load_sem.at[len(loads)])
    put_result.start()

    to_core.wait()

    def summed(n, at):
        return cv[core, at + n] + core_recv[at + n].astype(F32)

    first = []
    for d in range(1, 4):
        at = lax.rem(u + d, 4) * 16

        @pl.loop(0, 16)
        def _(n):
            s1[d - 1, n] = summed(n, at).astype(BF16)

        first.append(remote(s1.at[d - 1], r1.at[d - 1], first_device(d)))
        first[-1].start()

    @pl.loop(0, 16)
    def _(n):
        a1[n] = summed(n, u * 16)

    for copy in first:
        copy.wait()

    def second_sum(n):
        return a1[n] + r1[0, n].astype(F32) + r1[1, n].astype(F32) + r1[2, n].astype(F32)

    second = []
    for d in range(1, 4):
        at = lax.rem(v + d, 4) * 4
        for n in range(4):
            s2[d - 1, n] = second_sum(at + n).astype(BF16)
        second.append(remote(s2.at[d - 1], r2.at[d - 1], second_device(d)))
        second[-1].start()
    for n in range(4):
        a2[n] = second_sum(v * 4 + n)
    for copy in second:
        copy.wait()

    def third_sum(n):
        return a2[n] + r2[0, n].astype(F32) + r2[1, n].astype(F32) + r2[2, n].astype(F32)

    third = []
    for d in range(1, 4):
        s3[d - 1] = third_sum(lax.rem(z + d, 4)).astype(BF16)
        third.append(remote(s3.at[d - 1], r3.at[d - 1], depth_device(d)))
        third[-1].start()
    own = third_sum(z)
    for copy in third:
        copy.wait()
    own = own + r3[0].astype(F32) + r3[1].astype(F32) + r3[2].astype(F32)
    a3[...] = own
    last = []
    base = count[0]
    count[0] += 2
    for k in range(2):
        last.append(
            pltpu.make_async_remote_copy(
                src_ref=a3.at[72:80],
                dst_ref=out_peer.at[core],
                send_sem=send_sem.at[base + k],
                recv_sem=recv_sem.at[base + core],
                device_id=dest[k],
                device_id_type=MESH,
            )
        )
        last[-1].start()
    conv_cross = remote(a3, conv_peer, peer_core)
    conv_cross.start()
    conv_cross.wait()
    peer = conv_peer[...]
    first_core = core == 0
    low_half = jnp.where(first_core, own, peer)
    high_half = jnp.where(first_core, peer, own)
    gconv_out[:, 0:STEP] = jnp.where(first_core, low_half[0:36], low_half[36:72])
    gconv_out[:, STEP:HALF] = jnp.where(first_core, high_half[0:36], high_half[36:72])
    for copy in last:
        copy.wait_send()
    for k in range(2):
        pltpu.make_async_remote_copy(
            src_ref=a3.at[72:80],
            dst_ref=out_peer.at[k],
            send_sem=send_sem.at[base + k],
            recv_sem=recv_sem.at[base + k],
            device_id=source[k],
            device_id_type=MESH,
        ).wait_recv()
        gout_out[:, k * STEP : (k + 1) * STEP] = jnp.where(
            first_core, out_peer[k, 0:4], out_peer[k, 4:8]
        )
    put_result.wait()


COPIES = 56
VMEM = pltpu.VMEM
ANY = pl.BlockSpec(memory_space=pl.ANY)
INSIDE = pl.BlockSpec(memory_space=pltpu.VMEM)


def time_embed(time_steps, emb_width):
    half_width = emb_width // 2
    frequency = jnp.exp(
        -math.log(10000.0) * jnp.arange(half_width).astype(F32) / half_width
    )
    angles = time_steps.astype(F32)[:, None] * frequency[None, :]
    return jnp.concatenate([jnp.sin(angles), jnp.cos(angles)], axis=1).astype(BF16)


def shards(
    pixels,
    hidden,
    enc_gain,
    lengths,
    time_steps,
    attn_gain,
    w_query,
    w_key,
    w_value,
    w_out,
    w_time,
    w_conv,
    cotangent,
):
    small = jnp.concatenate(
        [
            enc_gain.astype(F32).reshape(8, CH),
            attn_gain.astype(F32).reshape(1, CH),
            time_embed(time_steps, TEMB).astype(F32),
        ],
        axis=0,
    )
    result, grad_conv, grad_out_t = pl.pallas_call(
        kernel,
        out_shape=(
            jax.ShapeDtypeStruct((PIX, HALF), BF16),
            jax.ShapeDtypeStruct((36, HALF), F32),
            jax.ShapeDtypeStruct((4, HALF), F32),
        ),
        in_specs=[
            pl.BlockSpec(memory_space=pltpu.SMEM),
            ANY,
            ANY,
            INSIDE,
            ANY,
            ANY,
            ANY,
            ANY,
            ANY,
            ANY,
            ANY,
        ],
        out_specs=(ANY, INSIDE, INSIDE),
        scratch_shapes=[
            VMEM((EXT, CH), BF16),
            VMEM((EXT, HALF), BF16),
            VMEM((8, PIECE, CH), BF16),
            VMEM((2, CH, HALF), BF16),
            VMEM((4096, HALF), BF16),
            VMEM((4096, HALF), BF16),
            VMEM((2, HALF, CH), BF16),
            VMEM((TEMB, 2 * CH), BF16),
            VMEM((9 * CH, HALF), BF16),
            VMEM((2, TOK, CH), BF16),
            VMEM((2, 2, 8, HALF), F32),
            VMEM((2, EXT, HALF), BF16),
            VMEM((2, EXT, HALF), F32),
            VMEM((3, EXT, CH), BF16),
            VMEM((3, EXT, HALF), BF16),
            VMEM((PIX, HALF), BF16),
            VMEM((PIX, HALF), BF16),
            VMEM((PIX, HALF), F32),
            VMEM((PIX, HALF), BF16),
            VMEM((2, 64, 80, STEP), F32),
            VMEM((64, 80, STEP), BF16),
            VMEM((64, 80, STEP), BF16),
            VMEM((3, 16, 80, STEP), BF16),
            VMEM((3, 16, 80, STEP), BF16),
            VMEM((16, 80, STEP), F32),
            VMEM((3, 4, 80, STEP), BF16),
            VMEM((3, 4, 80, STEP), BF16),
            VMEM((4, 80, STEP), F32),
            VMEM((3, 80, STEP), BF16),
            VMEM((3, 80, STEP), BF16),
            VMEM((80, STEP), F32),
            VMEM((80, STEP), F32),
            VMEM((2, 8, STEP), F32),
            pltpu.SemaphoreType.DMA((10,)),
            pltpu.SemaphoreType.DMA((COPIES,)),
            pltpu.SemaphoreType.DMA((COPIES,)),
        ],
        compiler_params=pltpu.CompilerParams(
            collective_id=0, has_side_effects=True, vmem_limit_bytes=60 * 1024 * 1024
        ),
        name="block",
    )(
        lengths,
        pixels.reshape(PIX, CH),
        hidden.reshape(TOK, CH),
        small,
        w_query,
        w_key,
        w_value,
        w_out,
        w_time,
        w_conv,
        cotangent.reshape(PIX, HALF),
    )
    return result.reshape(1, ROWS, COLS, HALF), grad_conv, grad_out_t


def solution(mesh):
    finer = Mesh(
        mesh.devices.reshape(4, 4, 4, 2, mesh.shape["chan"]),
        ("dp_0", "dp_1", "space_0", "space_1", "chan"),
    )
    placed = (
        P(DP, SPACE, None, None),
        P(DP, None, SPACE),
        P(),
        P(DP),
        P(DP),
        P(),
        P(None, "chan"),
        P(None, "chan"),
        P(None, "chan"),
        P("chan", None),
        P(),
        P(None, "chan"),
        P(DP, SPACE, None, "chan"),
    )
    return jax.shard_map(
        shards,
        mesh=finer,
        in_specs=placed,
        out_specs=(P(DP, SPACE, None, "chan"), P(DP_SPACE, "chan"), P(DP_SPACE, "chan")),
        check_vma=False,
    )
```

```python
import math

import jax
import jax.numpy as jnp
from jax import lax
from jax.experimental import pallas as pl
from jax.experimental.pallas import tpu as pltpu
from jax.sharding import Mesh
from jax.sharding import PartitionSpec as P

TEMB = 512
SPACE = ("space_0", "space_1")
DP_SPACE = ("dp_0", "dp_1", "space_0", "space_1")
DP = ("dp_0", "dp_1")
F32 = jnp.float32
BF16 = jnp.bfloat16
MESH = pl.DeviceIdType.MESH

ROWS = 8
COLS = 64
PIX = ROWS * COLS
EXT = PIX + 2 * COLS
CH = 512
HALF = 256
TOK = 128
PIECE = 16
STEP = 128


def dot(a, b):
    return jnp.dot(a, b, preferred_element_type=F32)


def dot_nt(a, b):
    return lax.dot_general(a, b, (((1,), (1,)), ((), ())), preferred_element_type=F32)


def dot_tn(a, b):
    return lax.dot_general(a, b, (((0,), (0,)), ((), ())), preferred_element_type=F32)


def silu_gate(lifted):
    return 1.0 / (1.0 + jnp.exp(-lifted))


def shifted_columns(wide, store):
    col = lax.rem(lax.broadcasted_iota(jnp.int32, wide.shape, 0), COLS)
    down = pltpu.roll(wide, 1, 0)
    up = pltpu.roll(wide, wide.shape[0] - 1, 0)
    store(0, jnp.where(col == 0, 0.0, down).astype(BF16))
    store(1, wide.astype(BF16))
    store(2, jnp.where(col == COLS - 1, 0.0, up).astype(BF16))


def block_rows(tap):
    pieces = []
    row = tap * CH
    while row < (tap + 1) * CH:
        block, inside = divmod(row, 72)
        count = min(72 - inside, (tap + 1) * CH - row)
        pieces.append((block, inside, row - tap * CH, count))
        row += count
    return pieces


def place_of(half, block):
    x, z, y = block // 16, (block // 4) % 4, block % 4
    u, v = (x, y) if half == 0 else (y, x)
    return (z // 2) * 32 + u * 8 + v * 2 + z % 2


def whole_place(half, block):
    x, z, y = block // 16, (block // 4) % 4, block % 4
    u, v = (x, y) if half == 0 else (y, x)
    return u * 16 + v * 4 + z


def kernel(
    lengths,
    pix_in,
    hid_in,
    enc_in,
    attn_in,
    time_in,
    wq_in,
    wk_in,
    wv_in,
    wo_in,
    wt_in,
    wc_in,
    cot_in,
    res_out,
    gconv_out,
    gout_out,
    pix,
    cot,
    hid_own,
    hid,
    wq,
    wk,
    wv,
    wo,
    wt,
    wc,
    kv,
    film,
    normed,
    query,
    att,
    mix,
    act3,
    cot3,
    gact_send,
    gact_recv,
    gact_own,
    gmix,
    result,
    cv,
    core_send,
    core_recv,
    s1,
    r1,
    a1,
    s2,
    r2,
    a2,
    s3,
    r3,
    a3,
    conv_peer,
    ov,
    core_send_o,
    core_recv_o,
    s1o,
    r1o,
    a1o,
    s2o,
    r2o,
    a2o,
    s3o,
    r3o,
    a3o,
    out_peer,
    load_sem,
    send_sem,
    recv_sem,
):
    x = lax.axis_index("dp_0")
    z = lax.axis_index("dp_1")
    y = lax.axis_index("space_0")
    core = lax.axis_index("space_1")
    chan = lax.axis_index("chan")
    other = 1 - chan
    slab = y * 2 + core
    piece = x * 2 + core
    count = [0]

    def remote(src, dst, device):
        i = count[0]
        count[0] += 1
        return pltpu.make_async_remote_copy(
            src_ref=src,
            dst_ref=dst,
            send_sem=send_sem.at[i],
            recv_sem=recv_sem.at[i],
            device_id=device,
            device_id_type=MESH,
        )

    def slab_device(d):
        s = lax.rem(slab + d, 8)
        return {"space_0": s // 2, "space_1": lax.rem(s, 2)}

    u = x * (1 - core) + y * core
    v = y * (1 - core) + x * core

    def first_device(d):
        t = lax.rem(u + d, 4)
        return {"dp_0": t * (1 - core) + x * core, "space_0": y * (1 - core) + t * core}

    def second_device(d):
        t = lax.rem(v + d, 4)
        return {"dp_0": x * (1 - core) + t * core, "space_0": t * (1 - core) + y * core}

    def depth_device(d):
        return {"dp_1": lax.rem(z + d, 4)}

    peer_chan = {"chan": other}
    peer_core = {"space_1": 1 - core}
    half_x, low_x = x // 2, lax.rem(x, 2)
    dest = [{"dp_0": 2 * chan + low_x, "space_1": k, "chan": 1 - half_x} for k in range(2)]
    source = [{"dp_0": 2 * (1 - chan) + low_x, "space_1": k, "chan": half_x} for k in range(2)]

    def piece_device(d):
        p = lax.rem(piece + d, 8)
        return {"dp_0": p // 2, "space_1": lax.rem(p, 2)}

    barrier = pltpu.get_barrier_semaphore()
    greeted = (
        [peer_chan]
        + dest
        + source
        + [depth_device(d) for d in range(1, 4)]
        + [piece_device(d) for d in range(1, 8)]
        + [slab_device(d) for d in range(1, 8)]
    )
    for device in greeted:
        pl.semaphore_signal(barrier, inc=1, device_id=device, device_id_type=MESH)

    loads = []

    def load(src, dst):
        copy = pltpu.make_async_copy(src, dst, load_sem.at[len(loads)])
        copy.start()
        loads.append(copy)
        return copy

    ld_hid = load(hid_in, hid_own)
    ld_pix = load(pix_in, pix.at[COLS : COLS + PIX, :])
    ld_wq = load(wq_in, wq.at[chan])
    ld_cot = load(cot_in, cot.at[COLS : COLS + PIX, :])
    ld_wc = load(wc_in, wc)
    ld_wk = load(wk_in, wk)
    ld_wv = load(wv_in, wv)
    ld_wo = load(wo_in, wo.at[chan])
    ld_wt = load(wt_in, wt)

    top = (slab > 0).astype(F32)
    bottom = (slab < 7).astype(F32)
    attn = attn_in[...].astype(F32)
    attn_row = jnp.concatenate([attn[i : i + 1, :] for i in range(4)], axis=1)

    def query_rows(rows):
        part = pix[rows, :].astype(F32)
        mean = jnp.sum(part * part, axis=-1, keepdims=True) / 512.0
        norm = (part * lax.rsqrt(mean + 1e-06) * attn_row).astype(BF16)
        normed[rows, :] = norm
        query[chan, rows, :] = dot(norm, wq[chan]).astype(BF16)

    ld_pix.wait()
    ld_wq.wait()

    @pl.loop(0, PIX // STEP)
    def _(m):
        query_rows(pl.ds(pl.multiple_of(m * STEP + COLS, COLS), STEP))

    ld_hid.wait()
    ld_cot.wait()
    pl.semaphore_wait(barrier, len(greeted))

    hid_copies = []
    for d in range(1, 8):
        s = lax.rem(slab + d, 8)
        there = pl.ds(pl.multiple_of(s * PIECE, PIECE), PIECE)
        hid_copies.append(remote(hid_own.at[there, :], hid.at[slab], slab_device(d)))
        hid_copies[-1].start()
    wq_rows = pl.ds(pl.multiple_of(piece * 64, 64), 64)
    wo_rows = pl.ds(pl.multiple_of(piece * 32, 32), 32)
    w_copies = [
        remote(wq_in.at[wq_rows, :], wq.at[chan, wq_rows, :], peer_chan),
        remote(wo_in.at[wo_rows, :], wo.at[chan, wo_rows, :], peer_chan),
    ]
    for copy in w_copies:
        copy.start()
    halos = [
        remote(pix.at[PIX : PIX + COLS, :], pix.at[0:COLS, :], slab_device(1)),
        remote(pix.at[COLS : 2 * COLS, :], pix.at[COLS + PIX : EXT, :], slab_device(7)),
        remote(cot.at[PIX : PIX + COLS, :], cot.at[0:COLS, :], slab_device(1)),
        remote(cot.at[COLS : 2 * COLS, :], cot.at[COLS + PIX : EXT, :], slab_device(7)),
    ]
    for copy in halos:
        copy.start()

    def shift_cot(start, size, factor):
        wide = cot[start : start + size, :].astype(F32)
        if factor is not None:
            wide = wide * factor

        def put_cot(b, value):
            cot3[b, start : start + size, :] = value

        shifted_columns(wide, put_cot)

    shift_cot(COLS, PIX, None)
    ld_wc.wait()

    def grad_half(which, m):
        total = None
        for a in range(3):
            for b in range(3):
                tap = 3 * a + b
                left = cot3[2 - b, pl.ds(pl.multiple_of((2 - a) * COLS + m * STEP, COLS), STEP), :]
                rows = pl.ds(pl.multiple_of(tap * CH + which * HALF, HALF), HALF)
                term = dot_nt(left, wc[rows, :])
                total = term if total is None else total + term
        return total

    def grad_rows(m):
        rows = pl.ds(pl.multiple_of(m * STEP, STEP), STEP)
        gact_send[rows, :] = grad_half(other, m).astype(BF16)
        gact_own[rows, :] = grad_half(chan, m)

    @pl.loop(1, 3)
    def _(m):
        grad_rows(m)

    gact_inner = remote(
        gact_send.at[STEP : 3 * STEP, :], gact_recv.at[STEP : 3 * STEP, :], peer_chan
    )

    enc = enc_in[...].astype(F32)
    ld_wk.wait()
    ld_wv.wait()
    for copy in hid_copies:
        copy.wait()
    own_tokens = pl.ds(pl.multiple_of(slab * PIECE, PIECE), PIECE)
    hid[slab] = hid_own[own_tokens, :]
    squares = None
    for s in range(8):
        part = hid[s].astype(F32)
        part = jnp.sum(part * part, axis=-1, keepdims=True)
        squares = part if squares is None else squares + part
    scale = lax.rsqrt(squares / 4096.0 + 1e-06)
    key_sum, value_sum = None, None
    for s in range(8):
        gain = jnp.concatenate([enc[4 * s + i : 4 * s + i + 1, :] for i in range(4)], axis=1)
        context = (hid[s].astype(F32) * scale * gain).astype(BF16)
        key_part = dot(context, wk[s * CH : (s + 1) * CH, :])
        value_part = dot(context, wv[s * CH : (s + 1) * CH, :])
        key_sum = key_part if key_sum is None else key_sum + key_part
        value_sum = value_part if value_sum is None else value_sum + value_part
    kv[chan, own_tokens, 0:HALF] = key_sum.astype(BF16)
    kv[chan, own_tokens, HALF:CH] = value_sum.astype(BF16)
    kv_cross = remote(kv.at[chan, own_tokens, :], kv.at[chan, own_tokens, :], peer_chan)
    kv_cross.start()
    kv_copies = []
    for d in range(1, 8):
        kv_copies.append(
            remote(kv.at[chan, own_tokens, :], kv.at[chan, own_tokens, :], slab_device(d))
        )
        kv_copies[-1].start()
    gact_inner.start()

    w_spread = []
    for copy in w_copies:
        copy.wait()
    for d in range(1, 8):
        w_spread.append(
            remote(wq.at[other, wq_rows, :], wq.at[other, wq_rows, :], piece_device(d))
        )
        w_spread[-1].start()
    for d in range(1, 8):
        w_spread.append(
            remote(wo.at[other, wo_rows, :], wo.at[other, wo_rows, :], piece_device(d))
        )
        w_spread[-1].start()

    for copy in halos:
        copy.wait()
    query_rows(pl.ds(0, COLS))
    query_rows(pl.ds(COLS + PIX, COLS))
    shift_cot(0, COLS, top)
    shift_cot(COLS + PIX, COLS, bottom)

    @pl.loop(0, 2)
    def _(m):
        grad_rows(m * 3)

    gact_edges = [
        remote(gact_send.at[at : at + STEP, :], gact_recv.at[at : at + STEP, :], peer_chan)
        for at in (0, 3 * STEP)
    ]
    for copy in gact_edges:
        copy.start()

    kv_cross.wait()
    kv_spread = []
    for d in range(1, 8):
        kv_spread.append(
            remote(kv.at[other, own_tokens, :], kv.at[other, own_tokens, :], slab_device(d))
        )
        kv_spread[-1].start()

    ld_wt.wait()
    time_row = jnp.broadcast_to(time_in[...].astype(F32), (16, CH)).astype(BF16)
    film_rows = dot(time_row, wt[...])
    for h in range(2):
        film[h, 0] = film_rows[0:8, h * HALF : (h + 1) * HALF]
        film[h, 1] = film_rows[0:8, CH + h * HALF : CH + (h + 1) * HALF]

    ld_wo.wait()
    for copy in kv_copies:
        copy.wait()
    lane = lax.broadcasted_iota(jnp.int32, (TOK, STEP), 1)
    low_lanes = lane < 64
    live = lax.broadcasted_iota(jnp.int32, (STEP, TOK), 1) < lengths[0]
    zero = jnp.zeros((TOK, STEP), BF16)

    def attend(group, rows):
        for pair in range(2):
            at = pair * STEP
            keys = kv[group, :, at : at + STEP]
            values = kv[group, :, HALF + at : HALF + at + STEP]
            total = None
            for head in range(2):
                keep = low_lanes if head == 0 else jnp.logical_not(low_lanes)
                scores = dot_nt(query[group, rows, at : at + STEP], jnp.where(keep, keys, zero))
                scores = jnp.where(live, scores * 0.125, -1e30)
                peak = jnp.max(scores, axis=-1, keepdims=True)
                raised = jnp.exp(scores - peak)
                soft = raised / jnp.sum(raised, axis=-1, keepdims=True)
                term = dot(soft.astype(BF16), jnp.where(keep, values, zero))
                total = term if total is None else total + term
            att[group, rows, at : at + STEP] = total.astype(BF16)

    @pl.loop(0, EXT // STEP)
    def _(m):
        rows = pl.ds(pl.multiple_of(m * STEP, STEP), STEP)
        attend(chan, rows)
        mixed = pix[rows, :].astype(F32) + dot(att[chan, rows, :], wo[chan])
        mix[0, rows, :] = mixed[:, 0:HALF]
        mix[1, rows, :] = mixed[:, HALF:CH]

    for copy in w_spread:
        copy.wait()

    @pl.loop(0, EXT // STEP)
    def _(m):
        rows = pl.ds(pl.multiple_of(m * STEP, STEP), STEP)
        query[other, rows, :] = dot(normed[rows, :], wq[other]).astype(BF16)

    for copy in kv_spread:
        copy.wait()

    @pl.loop(0, EXT // STEP)
    def _(m):
        rows = pl.ds(pl.multiple_of(m * STEP, STEP), STEP)
        attend(other, rows)
        mixed = dot(att[other, rows, :], wo[other])
        mix[0, rows, :] += mixed[:, 0:HALF]
        mix[1, rows, :] += mixed[:, HALF:CH]

    for h in range(2):
        lifted = mix[h] * (1.0 + film[h, 0, 0:1, :]) + film[h, 1, 0:1, :]
        active = lifted * silu_gate(lifted)
        active = jnp.concatenate(
            [active[0:COLS] * top, active[COLS : COLS + PIX], active[COLS + PIX : EXT] * bottom],
            axis=0,
        )

        def put_act(b, value):
            act3[b, :, h * HALF : (h + 1) * HALF] = value

        shifted_columns(active.astype(BF16).astype(F32), put_act)

    for tap in range(9):
        a, b = divmod(tap, 3)
        term = dot_tn(act3[b, a * COLS : a * COLS + PIX, :], cot[COLS : COLS + PIX, :])
        for block, inside, row, size in block_rows(tap):
            for h in range(2):
                at = place_of(h, block) * 72 + inside
                cv[h, at : at + size, :] = term[row : row + size, h * STEP : (h + 1) * STEP]

    to_core = []
    for c in range(2):

        @pl.loop(0, 2304 // 144)
        def _(i):
            rows = pl.ds(pl.multiple_of(c * 2304 + i * 144, 16), 144)
            core_send[rows, :] = cv[1 - core, rows, :].astype(BF16)

        rows = slice(c * 2304, (c + 1) * 2304)
        to_core.append(remote(core_send.at[rows, :], core_recv.at[rows, :], peer_core))
        to_core[-1].start()

    gact_inner.wait()
    for copy in gact_edges:
        copy.wait()

    @pl.loop(0, PIX // STEP)
    def _(m):
        rows = pl.ds(pl.multiple_of(m * STEP, STEP), STEP)
        rows_ext = pl.ds(pl.multiple_of(m * STEP + COLS, COLS), STEP)
        gain = 1.0 + film[chan, 0, 0:1, :]
        lifted = mix[chan, rows_ext, :] * gain + film[chan, 1, 0:1, :]
        gate = silu_gate(lifted)
        grad_act = gact_own[rows, :] + gact_recv[rows, :].astype(F32)
        grad_lift = grad_act * gate * (1.0 + lifted * (1.0 - gate))
        gmix[rows, :] = (cot[rows_ext, :].astype(F32) + grad_lift * gain).astype(BF16)

    for to in range(2):
        term = dot_tn(gmix[...], att[to, COLS : COLS + PIX, :])
        for low in range(2):
            for zz in range(4):
                for yy in range(4):
                    row = low * 128 + zz * 32 + yy * 8
                    block = (2 * (1 - to) + low) * 16 + zz * 4 + yy
                    for h in range(2):
                        at = whole_place(h, block) * 8
                        ov[h, at : at + 8, :] = term[row : row + 8, h * STEP : (h + 1) * STEP]
    core_send_o[...] = ov[1 - core].astype(BF16)
    to_core_o = remote(core_send_o, core_recv_o, peer_core)
    to_core_o.start()

    first = [[], []]

    def first_stage(c):
        to_core[c].wait()
        for d in range(1, 4):
            start = c * 2304 + lax.rem(u + d, 4) * 576

            @pl.loop(0, 4)
            def _(i):
                rows = pl.ds(pl.multiple_of(start + i * 144, 16), 144)
                total = cv[core, rows, :] + core_recv[rows, :].astype(F32)
                s1[c, d - 1, pl.ds(pl.multiple_of(i * 144, 16), 144), :] = total.astype(BF16)

            first[c].append(remote(s1.at[c, d - 1], r1.at[c, d - 1], first_device(d)))
            first[c][-1].start()

    first_stage(0)
    to_core_o.wait()
    first_o = []
    for d in range(1, 4):
        rows = pl.ds(pl.multiple_of(lax.rem(u + d, 4) * 128, 128), 128)
        total = ov[core, rows, :] + core_recv_o[rows, :].astype(F32)
        s1o[d - 1] = total.astype(BF16)
        first_o.append(remote(s1o.at[d - 1], r1o.at[d - 1], first_device(d)))
        first_o[-1].start()
    first_stage(1)

    @pl.loop(0, PIX // STEP)
    def _(m):
        rows = pl.ds(pl.multiple_of(m * STEP, STEP), STEP)
        rows_ext = pl.ds(pl.multiple_of(m * STEP + COLS, COLS), STEP)
        total = mix[chan, rows_ext, :]
        for a in range(3):
            for b in range(3):
                tap = 3 * a + b
                left = act3[b, pl.ds(pl.multiple_of(a * COLS + m * STEP, COLS), STEP), :]
                total = total + dot(left, wc[tap * CH : (tap + 1) * CH, :])
        result[rows, :] = total.astype(BF16)

    put_result = pltpu.make_async_copy(result, res_out, load_sem.at[len(loads)])
    put_result.start()

    for c in range(2):

        @pl.loop(0, 4)
        def _(i):
            rows = pl.ds(pl.multiple_of(c * 2304 + u * 576 + i * 144, 16), 144)
            a1[c, pl.ds(pl.multiple_of(i * 144, 16), 144), :] = cv[core, rows, :] + core_recv[
                rows, :
            ].astype(F32)

    for copy in first_o:
        copy.wait()
    rows = pl.ds(pl.multiple_of(u * 128, 128), 128)
    a1o[...] = (
        ov[core, rows, :]
        + core_recv_o[rows, :].astype(F32)
        + r1o[0].astype(F32)
        + r1o[1].astype(F32)
        + r1o[2].astype(F32)
    )
    second_o = []
    for d in range(1, 4):
        rows = pl.ds(pl.multiple_of(lax.rem(v + d, 4) * 32, 32), 32)
        s2o[d - 1] = a1o[rows, :].astype(BF16)
        second_o.append(remote(s2o.at[d - 1], r2o.at[d - 1], second_device(d)))
        second_o[-1].start()

    second = [[], []]

    def second_stage(c):
        for copy in first[c]:
            copy.wait()

        def total(at):
            rows = pl.ds(pl.multiple_of(at * 144, 16), 144)
            return (
                a1[c, rows, :]
                + r1[c, 0, rows, :].astype(F32)
                + r1[c, 1, rows, :].astype(F32)
                + r1[c, 2, rows, :].astype(F32)
            )

        for d in range(1, 4):
            s2[c, d - 1] = total(lax.rem(v + d, 4)).astype(BF16)
            second[c].append(remote(s2.at[c, d - 1], r2.at[c, d - 1], second_device(d)))
            second[c][-1].start()
        a2[c] = total(v)

    second_stage(0)
    for copy in second_o:
        copy.wait()
    rows = pl.ds(pl.multiple_of(v * 32, 32), 32)
    a2o[...] = (
        a1o[rows, :] + r2o[0].astype(F32) + r2o[1].astype(F32) + r2o[2].astype(F32)
    )
    third_o = []
    for d in range(1, 4):
        rows = pl.ds(pl.multiple_of(lax.rem(z + d, 4) * 8, 8), 8)
        s3o[d - 1] = a2o[rows, :]
        third_o.append(remote(s3o.at[d - 1], r3o.at[d - 1], depth_device(d)))
        third_o[-1].start()
    second_stage(1)
    for copy in third_o:
        copy.wait()
    rows = pl.ds(pl.multiple_of(z * 8, 8), 8)
    a3o[...] = a2o[rows, :] + r3o[0] + r3o[1] + r3o[2]
    last = []
    base = count[0]
    count[0] += 2
    for k in range(2):
        last.append(
            pltpu.make_async_remote_copy(
                src_ref=a3o,
                dst_ref=out_peer.at[core],
                send_sem=send_sem.at[base + k],
                recv_sem=recv_sem.at[base + core],
                device_id=dest[k],
                device_id_type=MESH,
            )
        )
        last[-1].start()

    for c in range(2):
        for copy in second[c]:
            copy.wait()

    for c in range(2):
        a2[c] = (
            a2[c] + r2[c, 0].astype(F32) + r2[c, 1].astype(F32) + r2[c, 2].astype(F32)
        )

    def third_rows(t):
        rows = pl.ds(pl.multiple_of(lax.rem(t, 2) * 72, 8), 72)
        return a2[t // 2, rows, :]

    pad = jnp.zeros((8, STEP), F32)
    third = []
    for d in range(1, 4):
        total = third_rows(lax.rem(z + d, 4))
        s3[d - 1] = jnp.concatenate([total, pad], axis=0).astype(BF16)
        third.append(remote(s3.at[d - 1], r3.at[d - 1], depth_device(d)))
        third[-1].start()
    own = third_rows(z)
    for copy in third:
        copy.wait()
    arrived = r3[0].astype(F32) + r3[1].astype(F32) + r3[2].astype(F32)
    own = own + arrived[0:72]
    a3[...] = own
    conv_cross = remote(a3, conv_peer, peer_core)
    conv_cross.start()
    first_core = core == 0
    for copy in last:
        copy.wait_send()
    for k in range(2):
        pltpu.make_async_remote_copy(
            src_ref=a3o,
            dst_ref=out_peer.at[k],
            send_sem=send_sem.at[base + k],
            recv_sem=recv_sem.at[base + k],
            device_id=source[k],
            device_id_type=MESH,
        ).wait_recv()
        gout_out[:, k * STEP : (k + 1) * STEP] = jnp.where(
            first_core, out_peer[k, 0:4], out_peer[k, 4:8]
        )
    conv_cross.wait()
    peer = conv_peer[...]
    low_half = jnp.where(first_core, own, peer)
    high_half = jnp.where(first_core, peer, own)
    gconv_out[:, 0:STEP] = jnp.where(first_core, low_half[0:36], low_half[36:72])
    gconv_out[:, STEP:HALF] = jnp.where(first_core, high_half[0:36], high_half[36:72])
    put_result.wait()
    assert count[0] == COPIES


def output_kernel(a, b, c, a_out, b_out, c_out, sems):
    copies = [
        pltpu.make_async_copy(src, dst, sems.at[i])
        for i, (src, dst) in enumerate(((a, a_out), (b, b_out), (c, c_out)))
    ]
    for copy in copies:
        copy.start()
    for copy in copies:
        copy.wait()


COPIES = 75
VMEM = pltpu.VMEM
ANY = pl.BlockSpec(memory_space=pl.ANY)
INSIDE = pl.BlockSpec(memory_space=pltpu.VMEM)


def time_embed(time_steps, emb_width):
    half_width = emb_width // 2
    lane = jnp.arange(emb_width)
    place = lax.rem(lane, half_width).astype(F32)
    frequency = jnp.exp(-math.log(10000.0) * place / half_width)
    angles = time_steps.astype(F32)[:, None] * frequency[None, :]
    return jnp.where((lane < half_width)[None, :], jnp.sin(angles), jnp.cos(angles)).astype(BF16)


def shards(
    pixels,
    hidden,
    enc_gain,
    lengths,
    time_steps,
    attn_gain,
    w_query,
    w_key,
    w_value,
    w_out,
    w_time,
    w_conv,
    cotangent,
):
    time_row = time_embed(time_steps, TEMB)
    result, grad_conv, grad_out_t = pl.pallas_call(
        kernel,
        out_shape=(
            jax.ShapeDtypeStruct((PIX, HALF), BF16),
            jax.ShapeDtypeStruct((36, HALF), F32),
            jax.ShapeDtypeStruct((4, HALF), F32),
        ),
        in_specs=[
            pl.BlockSpec(memory_space=pltpu.SMEM),
            ANY,
            ANY,
            INSIDE,
            INSIDE,
            INSIDE,
            ANY,
            ANY,
            ANY,
            ANY,
            ANY,
            ANY,
            ANY,
        ],
        out_specs=(ANY, INSIDE, INSIDE),
        scratch_shapes=[
            VMEM((EXT, CH), BF16),
            VMEM((EXT, HALF), BF16),
            VMEM((TOK, CH), BF16),
            VMEM((8, PIECE, CH), BF16),
            VMEM((2, CH, HALF), BF16),
            VMEM((4096, HALF), BF16),
            VMEM((4096, HALF), BF16),
            VMEM((2, HALF, CH), BF16),
            VMEM((TEMB, 2 * CH), BF16),
            VMEM((9 * CH, HALF), BF16),
            VMEM((2, TOK, CH), BF16),
            VMEM((2, 2, 8, HALF), F32),
            VMEM((EXT, CH), BF16),
            VMEM((2, EXT, HALF), BF16),
            VMEM((2, EXT, HALF), BF16),
            VMEM((2, EXT, HALF), F32),
            VMEM((3, EXT, CH), BF16),
            VMEM((3, EXT, HALF), BF16),
            VMEM((PIX, HALF), BF16),
            VMEM((PIX, HALF), BF16),
            VMEM((PIX, HALF), F32),
            VMEM((PIX, HALF), BF16),
            VMEM((PIX, HALF), BF16),
            VMEM((2, 4608, STEP), F32),
            VMEM((4608, STEP), BF16),
            VMEM((4608, STEP), BF16),
            VMEM((2, 3, 576, STEP), BF16),
            VMEM((2, 3, 576, STEP), BF16),
            VMEM((2, 576, STEP), F32),
            VMEM((2, 3, 144, STEP), BF16),
            VMEM((2, 3, 144, STEP), BF16),
            VMEM((2, 144, STEP), F32),
            VMEM((3, 80, STEP), BF16),
            VMEM((3, 80, STEP), BF16),
            VMEM((72, STEP), F32),
            VMEM((72, STEP), F32),
            VMEM((2, 512, STEP), F32),
            VMEM((512, STEP), BF16),
            VMEM((512, STEP), BF16),
            VMEM((3, 128, STEP), BF16),
            VMEM((3, 128, STEP), BF16),
            VMEM((128, STEP), F32),
            VMEM((3, 32, STEP), BF16),
            VMEM((3, 32, STEP), BF16),
            VMEM((32, STEP), F32),
            VMEM((3, 8, STEP), F32),
            VMEM((3, 8, STEP), F32),
            VMEM((8, STEP), F32),
            VMEM((2, 8, STEP), F32),
            pltpu.SemaphoreType.DMA((10,)),
            pltpu.SemaphoreType.DMA((COPIES,)),
            pltpu.SemaphoreType.DMA((COPIES,)),
        ],
        compiler_params=pltpu.CompilerParams(
            collective_id=0, has_side_effects=True, vmem_limit_bytes=60 * 1024 * 1024
        ),
        name="block",
    )(
        lengths,
        pixels.reshape(PIX, CH),
        hidden.reshape(TOK, CH),
        enc_gain.reshape(32, STEP),
        attn_gain.reshape(4, STEP),
        time_row,
        w_query,
        w_key,
        w_value,
        w_out,
        w_time,
        w_conv,
        cotangent.reshape(PIX, HALF),
    )
    result, grad_conv, grad_out_t = pl.pallas_call(
        output_kernel,
        out_shape=(
            jax.ShapeDtypeStruct((PIX, HALF), BF16),
            jax.ShapeDtypeStruct((36, HALF), F32),
            jax.ShapeDtypeStruct((4, HALF), F32),
        ),
        in_specs=[ANY] * 3,
        out_specs=(INSIDE,) * 3,
        scratch_shapes=[pltpu.SemaphoreType.DMA((3,))],
        compiler_params=pltpu.CompilerParams(vmem_limit_bytes=60 * 1024 * 1024),
        name="outputs",
    )(result, grad_conv, grad_out_t)
    return result.reshape(1, ROWS, COLS, HALF), grad_conv, grad_out_t


def solution(mesh):
    finer = Mesh(
        mesh.devices.reshape(4, 4, 4, 2, mesh.shape["chan"]),
        ("dp_0", "dp_1", "space_0", "space_1", "chan"),
    )
    placed = (
        P(DP, SPACE, None, None),
        P(DP, None, SPACE),
        P(),
        P(DP),
        P(DP),
        P(),
        P(None, "chan"),
        P(None, "chan"),
        P(None, "chan"),
        P("chan", None),
        P(),
        P(None, "chan"),
        P(DP, SPACE, None, "chan"),
    )
    return jax.shard_map(
        shards,
        mesh=finer,
        in_specs=placed,
        out_specs=(P(DP, SPACE, None, "chan"), P(DP_SPACE, "chan"), P(DP_SPACE, "chan")),
        check_vma=False,
    )
```

```python
import math

import jax
import jax.numpy as jnp
from jax import lax
from jax.experimental import pallas as pl
from jax.experimental.pallas import tpu as pltpu
from jax.sharding import Mesh
from jax.sharding import PartitionSpec as P

TEMB = 512
SPACE = ("space_0", "space_1")
DP_SPACE = ("dp_0", "dp_1", "space_0", "space_1")
DP = ("dp_0", "dp_1")
F32 = jnp.float32
BF16 = jnp.bfloat16
MESH = pl.DeviceIdType.MESH

ROWS = 8
COLS = 64
PIX = ROWS * COLS
EXT = PIX + 2 * COLS
CH = 512
HALF = 256
TOK = 128
PIECE = 16
STEP = 128


def dot(a, b):
    return jnp.dot(a, b, preferred_element_type=F32)


def dot_nt(a, b):
    return lax.dot_general(a, b, (((1,), (1,)), ((), ())), preferred_element_type=F32)


def dot_tn(a, b):
    return lax.dot_general(a, b, (((0,), (0,)), ((), ())), preferred_element_type=F32)


def silu_gate(lifted):
    return 1.0 / (1.0 + jnp.exp(-lifted))


def shifted_columns(wide, store):
    col = lax.rem(lax.broadcasted_iota(jnp.int32, wide.shape, 0), COLS)
    down = pltpu.roll(wide, 1, 0)
    up = pltpu.roll(wide, wide.shape[0] - 1, 0)
    store(0, jnp.where(col == 0, 0.0, down).astype(BF16))
    store(1, wide.astype(BF16))
    store(2, jnp.where(col == COLS - 1, 0.0, up).astype(BF16))


def block_rows(tap):
    pieces = []
    row = tap * CH
    while row < (tap + 1) * CH:
        block, inside = divmod(row, 72)
        count = min(72 - inside, (tap + 1) * CH - row)
        pieces.append((block, inside, row - tap * CH, count))
        row += count
    return pieces


def place_of(half, block):
    x, z, y = block // 16, (block // 4) % 4, block % 4
    u, v = (x, y) if half == 0 else (y, x)
    return (z // 2) * 32 + u * 8 + v * 2 + z % 2


def whole_place(half, block):
    x, z, y = block // 16, (block // 4) % 4, block % 4
    u, v = (x, y) if half == 0 else (y, x)
    return u * 16 + v * 4 + z


def kernel(
    lengths,
    pix_in,
    hid_in,
    enc_in,
    attn_in,
    time_in,
    wq_in,
    wk_in,
    wv_in,
    wo_in,
    wt_in,
    wc_in,
    cot_in,
    res_out,
    gconv_out,
    gout_out,
    pix,
    cot,
    hid_own,
    hid,
    wq,
    wk,
    wv,
    wo,
    wt,
    wc,
    kv,
    film,
    normed,
    query,
    att,
    mix,
    act3,
    cot3,
    gact_send,
    gact_recv,
    gact_own,
    gmix,
    result,
    cv,
    core_send,
    core_recv,
    s1,
    r1,
    a1,
    s2,
    r2,
    a2,
    s3,
    r3,
    ov,
    core_send_o,
    core_recv_o,
    s1o,
    r1o,
    a1o,
    s2o,
    r2o,
    a2o,
    s3o,
    r3o,
    a3o,
    out_peer,
    load_sem,
    send_sem,
    recv_sem,
):
    x = lax.axis_index("dp_0")
    z = lax.axis_index("dp_1")
    y = lax.axis_index("space_0")
    core = lax.axis_index("space_1")
    chan = lax.axis_index("chan")
    other = 1 - chan
    slab = y * 2 + core
    piece = x * 2 + core
    count = [0]

    def remote(src, dst, device):
        i = count[0]
        count[0] += 1
        return pltpu.make_async_remote_copy(
            src_ref=src,
            dst_ref=dst,
            send_sem=send_sem.at[i],
            recv_sem=recv_sem.at[i],
            device_id=device,
            device_id_type=MESH,
        )

    def slab_device(d):
        s = lax.rem(slab + d, 8)
        return {"space_0": s // 2, "space_1": lax.rem(s, 2)}

    u = x * (1 - core) + y * core
    v = y * (1 - core) + x * core

    def first_device(d):
        t = lax.rem(u + d, 4)
        return {"dp_0": t * (1 - core) + x * core, "space_0": y * (1 - core) + t * core}

    def second_device(d):
        t = lax.rem(v + d, 4)
        return {"dp_0": x * (1 - core) + t * core, "space_0": t * (1 - core) + y * core}

    def depth_core_device(d, k):
        return {"dp_1": lax.rem(z + d, 4), "space_1": k}

    def depth_device(d):
        return {"dp_1": lax.rem(z + d, 4)}

    peer_chan = {"chan": other}
    peer_core = {"space_1": 1 - core}
    half_x, low_x = x // 2, lax.rem(x, 2)
    dest = [{"dp_0": 2 * chan + low_x, "space_1": k, "chan": 1 - half_x} for k in range(2)]
    source = [{"dp_0": 2 * (1 - chan) + low_x, "space_1": k, "chan": half_x} for k in range(2)]

    def piece_device(d):
        p = lax.rem(piece + d, 8)
        return {"dp_0": p // 2, "space_1": lax.rem(p, 2)}

    barrier = pltpu.get_barrier_semaphore()
    greeted = (
        [peer_chan]
        + dest
        + source
        + [depth_device(d) for d in range(1, 4)]
        + [depth_core_device(d, 1 - core) for d in range(1, 4)]
        + [piece_device(d) for d in range(1, 8)]
        + [slab_device(d) for d in range(1, 8)]
    )
    for device in greeted:
        pl.semaphore_signal(barrier, inc=1, device_id=device, device_id_type=MESH)

    loads = []

    def load(src, dst):
        copy = pltpu.make_async_copy(src, dst, load_sem.at[len(loads)])
        copy.start()
        loads.append(copy)
        return copy

    ld_hid = load(hid_in, hid_own)
    ld_pix = load(pix_in, pix.at[COLS : COLS + PIX, :])
    ld_wq = load(wq_in, wq.at[chan])
    ld_cot = load(cot_in, cot.at[COLS : COLS + PIX, :])
    ld_wc = load(wc_in, wc)
    ld_wk = load(wk_in, wk)
    ld_wv = load(wv_in, wv)
    ld_wo = load(wo_in, wo.at[chan])
    ld_wt = load(wt_in, wt)

    top = (slab > 0).astype(F32)
    bottom = (slab < 7).astype(F32)
    attn = attn_in[...].astype(F32)
    attn_row = jnp.concatenate([attn[i : i + 1, :] for i in range(4)], axis=1)

    def query_rows(rows):
        part = pix[rows, :].astype(F32)
        mean = jnp.sum(part * part, axis=-1, keepdims=True) / 512.0
        norm = (part * lax.rsqrt(mean + 1e-06) * attn_row).astype(BF16)
        normed[rows, :] = norm
        query[chan, rows, :] = dot(norm, wq[chan]).astype(BF16)

    ld_pix.wait()
    ld_wq.wait()

    @pl.loop(0, PIX // STEP)
    def _(m):
        query_rows(pl.ds(pl.multiple_of(m * STEP + COLS, COLS), STEP))

    ld_hid.wait()
    ld_cot.wait()
    pl.semaphore_wait(barrier, len(greeted))

    hid_copies = []
    for d in range(1, 8):
        s = lax.rem(slab + d, 8)
        there = pl.ds(pl.multiple_of(s * PIECE, PIECE), PIECE)
        hid_copies.append(remote(hid_own.at[there, :], hid.at[slab], slab_device(d)))
        hid_copies[-1].start()
    wq_rows = pl.ds(pl.multiple_of(piece * 64, 64), 64)
    wo_rows = pl.ds(pl.multiple_of(piece * 32, 32), 32)
    w_copies = [
        remote(wq_in.at[wq_rows, :], wq.at[chan, wq_rows, :], peer_chan),
        remote(wo_in.at[wo_rows, :], wo.at[chan, wo_rows, :], peer_chan),
    ]
    for copy in w_copies:
        copy.start()
    halos = [
        remote(pix.at[PIX : PIX + COLS, :], pix.at[0:COLS, :], slab_device(1)),
        remote(pix.at[COLS : 2 * COLS, :], pix.at[COLS + PIX : EXT, :], slab_device(7)),
        remote(cot.at[PIX : PIX + COLS, :], cot.at[0:COLS, :], slab_device(1)),
        remote(cot.at[COLS : 2 * COLS, :], cot.at[COLS + PIX : EXT, :], slab_device(7)),
    ]
    for copy in halos:
        copy.start()

    def shift_cot(start, size, factor):
        wide = cot[start : start + size, :].astype(F32)
        if factor is not None:
            wide = wide * factor

        def put_cot(b, value):
            cot3[b, start : start + size, :] = value

        shifted_columns(wide, put_cot)

    shift_cot(COLS, PIX, None)
    ld_wc.wait()

    def grad_half(which, m):
        total = None
        for a in range(3):
            for b in range(3):
                tap = 3 * a + b
                left = cot3[2 - b, pl.ds(pl.multiple_of((2 - a) * COLS + m * STEP, COLS), STEP), :]
                rows = pl.ds(pl.multiple_of(tap * CH + which * HALF, HALF), HALF)
                term = dot_nt(left, wc[rows, :])
                total = term if total is None else total + term
        return total

    def grad_rows(m):
        rows = pl.ds(pl.multiple_of(m * STEP, STEP), STEP)
        gact_send[rows, :] = grad_half(other, m).astype(BF16)
        gact_own[rows, :] = grad_half(chan, m)

    @pl.loop(1, 3)
    def _(m):
        grad_rows(m)

    gact_inner = remote(
        gact_send.at[STEP : 3 * STEP, :], gact_recv.at[STEP : 3 * STEP, :], peer_chan
    )

    enc = enc_in[...].astype(F32)
    ld_wk.wait()
    ld_wv.wait()
    w_spread = []
    w_copies[0].wait()
    for d in range(1, 8):
        w_spread.append(
            remote(wq.at[other, wq_rows, :], wq.at[other, wq_rows, :], piece_device(d))
        )
        w_spread[-1].start()
    for copy in hid_copies:
        copy.wait()
    own_tokens = pl.ds(pl.multiple_of(slab * PIECE, PIECE), PIECE)
    hid[slab] = hid_own[own_tokens, :]
    squares = None
    for s in range(8):
        part = hid[s].astype(F32)
        part = jnp.sum(part * part, axis=-1, keepdims=True)
        squares = part if squares is None else squares + part
    scale = lax.rsqrt(squares / 4096.0 + 1e-06)
    key_sum, value_sum = None, None
    for s in range(8):
        gain = jnp.concatenate([enc[4 * s + i : 4 * s + i + 1, :] for i in range(4)], axis=1)
        context = (hid[s].astype(F32) * scale * gain).astype(BF16)
        key_part = dot(context, wk[s * CH : (s + 1) * CH, :])
        value_part = dot(context, wv[s * CH : (s + 1) * CH, :])
        key_sum = key_part if key_sum is None else key_sum + key_part
        value_sum = value_part if value_sum is None else value_sum + value_part
    kv[chan, own_tokens, 0:HALF] = key_sum.astype(BF16)
    kv[chan, own_tokens, HALF:CH] = value_sum.astype(BF16)
    kv_cross = remote(kv.at[chan, own_tokens, :], kv.at[chan, own_tokens, :], peer_chan)
    kv_cross.start()
    kv_copies = []
    for d in range(1, 8):
        kv_copies.append(
            remote(kv.at[chan, own_tokens, :], kv.at[chan, own_tokens, :], slab_device(d))
        )
        kv_copies[-1].start()
    gact_inner.start()

    w_copies[1].wait()
    for d in range(1, 8):
        w_spread.append(
            remote(wo.at[other, wo_rows, :], wo.at[other, wo_rows, :], piece_device(d))
        )
        w_spread[-1].start()

    for copy in halos:
        copy.wait()
    query_rows(pl.ds(0, COLS))
    query_rows(pl.ds(COLS + PIX, COLS))
    shift_cot(0, COLS, top)
    shift_cot(COLS + PIX, COLS, bottom)

    @pl.loop(0, 2)
    def _(m):
        grad_rows(m * 3)

    gact_edges = [
        remote(gact_send.at[at : at + STEP, :], gact_recv.at[at : at + STEP, :], peer_chan)
        for at in (0, 3 * STEP)
    ]
    for copy in gact_edges:
        copy.start()

    kv_cross.wait()
    kv_spread = []
    for d in range(1, 8):
        kv_spread.append(
            remote(kv.at[other, own_tokens, :], kv.at[other, own_tokens, :], slab_device(d))
        )
        kv_spread[-1].start()

    ld_wt.wait()
    time_row = jnp.broadcast_to(time_in[...].astype(F32), (16, CH)).astype(BF16)
    film_rows = dot(time_row, wt[...])
    for h in range(2):
        film[h, 0] = film_rows[0:8, h * HALF : (h + 1) * HALF]
        film[h, 1] = film_rows[0:8, CH + h * HALF : CH + (h + 1) * HALF]

    ld_wo.wait()
    for copy in kv_copies:
        copy.wait()
    lane = lax.broadcasted_iota(jnp.int32, (TOK, STEP), 1)
    low_lanes = lane < 64
    live = lax.broadcasted_iota(jnp.int32, (STEP, TOK), 1) < lengths[0]
    zero = jnp.zeros((TOK, STEP), BF16)

    def attend(group, rows):
        for pair in range(2):
            at = pair * STEP
            keys = kv[group, :, at : at + STEP]
            values = kv[group, :, HALF + at : HALF + at + STEP]
            total = None
            for head in range(2):
                keep = low_lanes if head == 0 else jnp.logical_not(low_lanes)
                scores = dot_nt(query[group, rows, at : at + STEP], jnp.where(keep, keys, zero))
                scores = jnp.where(live, scores * 0.125, -1e30)
                peak = jnp.max(scores, axis=-1, keepdims=True)
                raised = jnp.exp(scores - peak)
                soft = raised / jnp.sum(raised, axis=-1, keepdims=True)
                term = dot(soft.astype(BF16), jnp.where(keep, values, zero))
                total = term if total is None else total + term
            att[group, rows, at : at + STEP] = total.astype(BF16)

    @pl.loop(0, EXT // STEP)
    def _(m):
        rows = pl.ds(pl.multiple_of(m * STEP, STEP), STEP)
        attend(chan, rows)
        mixed = pix[rows, :].astype(F32) + dot(att[chan, rows, :], wo[chan])
        mix[0, rows, :] = mixed[:, 0:HALF]
        mix[1, rows, :] = mixed[:, HALF:CH]

    for copy in w_spread[:7]:
        copy.wait()

    @pl.loop(0, EXT // STEP)
    def _(m):
        rows = pl.ds(pl.multiple_of(m * STEP, STEP), STEP)
        query[other, rows, :] = dot(normed[rows, :], wq[other]).astype(BF16)

    for copy in kv_spread:
        copy.wait()
    for copy in w_spread[7:]:
        copy.wait()

    @pl.loop(0, EXT // STEP)
    def _(m):
        rows = pl.ds(pl.multiple_of(m * STEP, STEP), STEP)
        attend(other, rows)
        mixed = dot(att[other, rows, :], wo[other])
        mix[0, rows, :] += mixed[:, 0:HALF]
        mix[1, rows, :] += mixed[:, HALF:CH]

    for h in range(2):
        lifted = mix[h] * (1.0 + film[h, 0, 0:1, :]) + film[h, 1, 0:1, :]
        active = lifted * silu_gate(lifted)
        active = jnp.concatenate(
            [active[0:COLS] * top, active[COLS : COLS + PIX], active[COLS + PIX : EXT] * bottom],
            axis=0,
        )

        def put_act(b, value):
            act3[b, :, h * HALF : (h + 1) * HALF] = value

        shifted_columns(active.astype(BF16).astype(F32), put_act)

    for tap in range(9):
        a, b = divmod(tap, 3)
        term = dot_tn(act3[b, a * COLS : a * COLS + PIX, :], cot[COLS : COLS + PIX, :])
        for block, inside, row, size in block_rows(tap):
            for h in range(2):
                at = place_of(h, block) * 72 + inside
                cv[h, at : at + size, :] = term[row : row + size, h * STEP : (h + 1) * STEP]

    to_core = []
    for c in range(2):

        @pl.loop(0, 2304 // 144)
        def _(i):
            rows = pl.ds(pl.multiple_of(c * 2304 + i * 144, 16), 144)
            core_send[rows, :] = cv[1 - core, rows, :].astype(BF16)

        rows = slice(c * 2304, (c + 1) * 2304)
        to_core.append(remote(core_send.at[rows, :], core_recv.at[rows, :], peer_core))
        to_core[-1].start()

    gact_inner.wait()
    for copy in gact_edges:
        copy.wait()

    @pl.loop(0, PIX // STEP)
    def _(m):
        rows = pl.ds(pl.multiple_of(m * STEP, STEP), STEP)
        rows_ext = pl.ds(pl.multiple_of(m * STEP + COLS, COLS), STEP)
        gain = 1.0 + film[chan, 0, 0:1, :]
        lifted = mix[chan, rows_ext, :] * gain + film[chan, 1, 0:1, :]
        gate = silu_gate(lifted)
        grad_act = gact_own[rows, :] + gact_recv[rows, :].astype(F32)
        grad_lift = grad_act * gate * (1.0 + lifted * (1.0 - gate))
        gmix[rows, :] = (cot[rows_ext, :].astype(F32) + grad_lift * gain).astype(BF16)

    for to in range(2):
        term = dot_tn(gmix[...], att[to, COLS : COLS + PIX, :])
        for low in range(2):
            for zz in range(4):
                for yy in range(4):
                    row = low * 128 + zz * 32 + yy * 8
                    block = (2 * (1 - to) + low) * 16 + zz * 4 + yy
                    for h in range(2):
                        at = whole_place(h, block) * 8
                        ov[h, at : at + 8, :] = term[row : row + 8, h * STEP : (h + 1) * STEP]
    core_send_o[...] = ov[1 - core].astype(BF16)
    to_core_o = remote(core_send_o, core_recv_o, peer_core)
    to_core_o.start()

    first = [[], []]

    def first_stage(c):
        to_core[c].wait()
        for d in range(1, 4):
            start = c * 2304 + lax.rem(u + d, 4) * 576

            @pl.loop(0, 4)
            def _(i):
                rows = pl.ds(pl.multiple_of(start + i * 144, 16), 144)
                total = cv[core, rows, :] + core_recv[rows, :].astype(F32)
                s1[c, d - 1, pl.ds(pl.multiple_of(i * 144, 16), 144), :] = total.astype(BF16)

            first[c].append(remote(s1.at[c, d - 1], r1.at[c, d - 1], first_device(d)))
            first[c][-1].start()

    first_stage(0)
    to_core_o.wait()
    first_o = []
    for d in range(1, 4):
        rows = pl.ds(pl.multiple_of(lax.rem(u + d, 4) * 128, 128), 128)
        total = ov[core, rows, :] + core_recv_o[rows, :].astype(F32)
        s1o[d - 1] = total.astype(BF16)
        first_o.append(remote(s1o.at[d - 1], r1o.at[d - 1], first_device(d)))
        first_o[-1].start()
    first_stage(1)

    @pl.loop(0, PIX // STEP)
    def _(m):
        rows = pl.ds(pl.multiple_of(m * STEP, STEP), STEP)
        rows_ext = pl.ds(pl.multiple_of(m * STEP + COLS, COLS), STEP)
        total = mix[chan, rows_ext, :]
        for a in range(3):
            for b in range(3):
                tap = 3 * a + b
                left = act3[b, pl.ds(pl.multiple_of(a * COLS + m * STEP, COLS), STEP), :]
                total = total + dot(left, wc[tap * CH : (tap + 1) * CH, :])
        result[rows, :] = total.astype(BF16)

    put_result = pltpu.make_async_copy(result, res_out, load_sem.at[len(loads)])
    put_result.start()

    for c in range(2):

        @pl.loop(0, 4)
        def _(i):
            rows = pl.ds(pl.multiple_of(c * 2304 + u * 576 + i * 144, 16), 144)
            a1[c, pl.ds(pl.multiple_of(i * 144, 16), 144), :] = cv[core, rows, :] + core_recv[
                rows, :
            ].astype(F32)

    for copy in first_o:
        copy.wait()
    rows = pl.ds(pl.multiple_of(u * 128, 128), 128)
    a1o[...] = (
        ov[core, rows, :]
        + core_recv_o[rows, :].astype(F32)
        + r1o[0].astype(F32)
        + r1o[1].astype(F32)
        + r1o[2].astype(F32)
    )
    second_o = []
    for d in range(1, 4):
        rows = pl.ds(pl.multiple_of(lax.rem(v + d, 4) * 32, 32), 32)
        s2o[d - 1] = a1o[rows, :].astype(BF16)
        second_o.append(remote(s2o.at[d - 1], r2o.at[d - 1], second_device(d)))
        second_o[-1].start()

    second = [[], []]

    def second_total(c, at):
        rows = pl.ds(pl.multiple_of(at * 144, 16), 144)
        return (
            a1[c, rows, :]
            + r1[c, 0, rows, :].astype(F32)
            + r1[c, 1, rows, :].astype(F32)
            + r1[c, 2, rows, :].astype(F32)
        )

    def second_stage(c):
        for copy in first[c]:
            copy.wait()
        for d in range(1, 4):
            s2[c, d - 1] = second_total(c, lax.rem(v + d, 4)).astype(BF16)
            second[c].append(remote(s2.at[c, d - 1], r2.at[c, d - 1], second_device(d)))
            second[c][-1].start()

    second_stage(0)
    a2[0] = second_total(0, v)
    for copy in second_o:
        copy.wait()
    rows = pl.ds(pl.multiple_of(v * 32, 32), 32)
    a2o[...] = (
        a1o[rows, :] + r2o[0].astype(F32) + r2o[1].astype(F32) + r2o[2].astype(F32)
    )
    third_o = []
    for d in range(1, 4):
        rows = pl.ds(pl.multiple_of(lax.rem(z + d, 4) * 8, 8), 8)
        s3o[d - 1] = a2o[rows, :]
        third_o.append(remote(s3o.at[d - 1], r3o.at[d - 1], depth_device(d)))
        third_o[-1].start()
    second_stage(1)
    a2[1] = second_total(1, v)
    for copy in third_o:
        copy.wait()
    rows = pl.ds(pl.multiple_of(z * 8, 8), 8)
    a3o[...] = a2o[rows, :] + r3o[0] + r3o[1] + r3o[2]
    last = []
    base = count[0]
    count[0] += 2
    for k in range(2):
        last.append(
            pltpu.make_async_remote_copy(
                src_ref=a3o,
                dst_ref=out_peer.at[core],
                send_sem=send_sem.at[base + k],
                recv_sem=recv_sem.at[base + core],
                device_id=dest[k],
                device_id_type=MESH,
            )
        )
        last[-1].start()

    for c in range(2):
        for copy in second[c]:
            copy.wait()
        a2[c] = (
            a2[c] + r2[c, 0].astype(F32) + r2[c, 1].astype(F32) + r2[c, 2].astype(F32)
        )

    def third_rows(t, k):
        rows = pl.ds(pl.multiple_of(lax.rem(t, 2) * 72, 8), 72)
        total = a2[t // 2, rows, :]
        return jnp.where(k == 0, total[0:36], total[36:72])

    pad = jnp.zeros((12, STEP), F32)
    third = []
    for d in range(8):
        step, swap = d // 2, d % 2
        if d == 0:
            continue
        k = 1 - core if swap else core
        total = third_rows(lax.rem(z + step, 4), k)
        s3[d - 1] = jnp.concatenate([total, pad], axis=0).astype(BF16)
        third.append(remote(s3.at[d - 1], r3.at[d - 1], depth_core_device(step, k)))
        third[-1].start()
    own = third_rows(z, core)
    first_core = core == 0
    for copy in third:
        copy.wait()
    mine = own + r3[1].astype(F32)[0:36] + r3[3].astype(F32)[0:36] + r3[5].astype(F32)[0:36]
    cross = (
        r3[0].astype(F32) + r3[2].astype(F32) + r3[4].astype(F32) + r3[6].astype(F32)
    )[0:36]
    gconv_out[:, 0:STEP] = jnp.where(first_core, mine, cross)
    gconv_out[:, STEP:HALF] = jnp.where(first_core, cross, mine)
    for copy in last:
        copy.wait_send()
    for k in range(2):
        pltpu.make_async_remote_copy(
            src_ref=a3o,
            dst_ref=out_peer.at[k],
            send_sem=send_sem.at[base + k],
            recv_sem=recv_sem.at[base + k],
            device_id=source[k],
            device_id_type=MESH,
        ).wait_recv()
        gout_out[:, k * STEP : (k + 1) * STEP] = jnp.where(
            first_core, out_peer[k, 0:4], out_peer[k, 4:8]
        )
    put_result.wait()
    assert count[0] == COPIES


def output_kernel(a, b, c, a_out, b_out, c_out, sems):
    copies = [
        pltpu.make_async_copy(src, dst, sems.at[i])
        for i, (src, dst) in enumerate(((a, a_out), (b, b_out), (c, c_out)))
    ]
    for copy in copies:
        copy.start()
    for copy in copies:
        copy.wait()


COPIES = 78
VMEM = pltpu.VMEM
ANY = pl.BlockSpec(memory_space=pl.ANY)
INSIDE = pl.BlockSpec(memory_space=pltpu.VMEM)


def time_embed(time_steps, emb_width):
    half_width = emb_width // 2
    lane = jnp.arange(emb_width)
    place = lax.rem(lane, half_width).astype(F32)
    frequency = jnp.exp(-math.log(10000.0) * place / half_width)
    angles = time_steps.astype(F32)[:, None] * frequency[None, :]
    return jnp.where((lane < half_width)[None, :], jnp.sin(angles), jnp.cos(angles)).astype(BF16)


def shards(
    pixels,
    hidden,
    enc_gain,
    lengths,
    time_steps,
    attn_gain,
    w_query,
    w_key,
    w_value,
    w_out,
    w_time,
    w_conv,
    cotangent,
):
    time_row = time_embed(time_steps, TEMB)
    result, grad_conv, grad_out_t = pl.pallas_call(
        kernel,
        out_shape=(
            jax.ShapeDtypeStruct((PIX, HALF), BF16),
            jax.ShapeDtypeStruct((36, HALF), F32),
            jax.ShapeDtypeStruct((4, HALF), F32),
        ),
        in_specs=[
            pl.BlockSpec(memory_space=pltpu.SMEM),
            ANY,
            ANY,
            INSIDE,
            INSIDE,
            INSIDE,
            ANY,
            ANY,
            ANY,
            ANY,
            ANY,
            ANY,
            ANY,
        ],
        out_specs=(ANY, INSIDE, INSIDE),
        scratch_shapes=[
            VMEM((EXT, CH), BF16),
            VMEM((EXT, HALF), BF16),
            VMEM((TOK, CH), BF16),
            VMEM((8, PIECE, CH), BF16),
            VMEM((2, CH, HALF), BF16),
            VMEM((4096, HALF), BF16),
            VMEM((4096, HALF), BF16),
            VMEM((2, HALF, CH), BF16),
            VMEM((TEMB, 2 * CH), BF16),
            VMEM((9 * CH, HALF), BF16),
            VMEM((2, TOK, CH), BF16),
            VMEM((2, 2, 8, HALF), F32),
            VMEM((EXT, CH), BF16),
            VMEM((2, EXT, HALF), BF16),
            VMEM((2, EXT, HALF), BF16),
            VMEM((2, EXT, HALF), F32),
            VMEM((3, EXT, CH), BF16),
            VMEM((3, EXT, HALF), BF16),
            VMEM((PIX, HALF), BF16),
            VMEM((PIX, HALF), BF16),
            VMEM((PIX, HALF), F32),
            VMEM((PIX, HALF), BF16),
            VMEM((PIX, HALF), BF16),
            VMEM((2, 4608, STEP), F32),
            VMEM((4608, STEP), BF16),
            VMEM((4608, STEP), BF16),
            VMEM((2, 3, 576, STEP), BF16),
            VMEM((2, 3, 576, STEP), BF16),
            VMEM((2, 576, STEP), F32),
            VMEM((2, 3, 144, STEP), BF16),
            VMEM((2, 3, 144, STEP), BF16),
            VMEM((2, 144, STEP), F32),
            VMEM((7, 48, STEP), BF16),
            VMEM((7, 48, STEP), BF16),
            VMEM((2, 512, STEP), F32),
            VMEM((512, STEP), BF16),
            VMEM((512, STEP), BF16),
            VMEM((3, 128, STEP), BF16),
            VMEM((3, 128, STEP), BF16),
            VMEM((128, STEP), F32),
            VMEM((3, 32, STEP), BF16),
            VMEM((3, 32, STEP), BF16),
            VMEM((32, STEP), F32),
            VMEM((3, 8, STEP), F32),
            VMEM((3, 8, STEP), F32),
            VMEM((8, STEP), F32),
            VMEM((2, 8, STEP), F32),
            pltpu.SemaphoreType.DMA((10,)),
            pltpu.SemaphoreType.DMA((COPIES,)),
            pltpu.SemaphoreType.DMA((COPIES,)),
        ],
        compiler_params=pltpu.CompilerParams(
            collective_id=0, has_side_effects=True, vmem_limit_bytes=60 * 1024 * 1024
        ),
        name="block",
    )(
        lengths,
        pixels.reshape(PIX, CH),
        hidden.reshape(TOK, CH),
        enc_gain.reshape(32, STEP),
        attn_gain.reshape(4, STEP),
        time_row,
        w_query,
        w_key,
        w_value,
        w_out,
        w_time,
        w_conv,
        cotangent.reshape(PIX, HALF),
    )
    result, grad_conv, grad_out_t = pl.pallas_call(
        output_kernel,
        out_shape=(
            jax.ShapeDtypeStruct((PIX, HALF), BF16),
            jax.ShapeDtypeStruct((36, HALF), F32),
            jax.ShapeDtypeStruct((4, HALF), F32),
        ),
        in_specs=[ANY] * 3,
        out_specs=(INSIDE,) * 3,
        scratch_shapes=[pltpu.SemaphoreType.DMA((3,))],
        compiler_params=pltpu.CompilerParams(vmem_limit_bytes=60 * 1024 * 1024),
        name="outputs",
    )(result, grad_conv, grad_out_t)
    return result.reshape(1, ROWS, COLS, HALF), grad_conv, grad_out_t


def solution(mesh):
    finer = Mesh(
        mesh.devices.reshape(4, 4, 4, 2, mesh.shape["chan"]),
        ("dp_0", "dp_1", "space_0", "space_1", "chan"),
    )
    placed = (
        P(DP, SPACE, None, None),
        P(DP, None, SPACE),
        P(),
        P(DP),
        P(DP),
        P(),
        P(None, "chan"),
        P(None, "chan"),
        P(None, "chan"),
        P("chan", None),
        P(),
        P(None, "chan"),
        P(DP, SPACE, None, "chan"),
    )
    return jax.shard_map(
        shards,
        mesh=finer,
        in_specs=placed,
        out_specs=(P(DP, SPACE, None, "chan"), P(DP_SPACE, "chan"), P(DP_SPACE, "chan")),
        check_vma=False,
    )
```

```python
import math

import jax
import jax.numpy as jnp
from jax import lax
from jax.experimental import pallas as pl
from jax.experimental.pallas import tpu as pltpu
from jax.sharding import Mesh
from jax.sharding import PartitionSpec as P

TEMB = 512
SPACE = ("space_0", "space_1")
DP_SPACE = ("dp_0", "dp_1", "space_0", "space_1")
DP = ("dp_0", "dp_1")
F32 = jnp.float32
BF16 = jnp.bfloat16
MESH = pl.DeviceIdType.MESH

ROWS = 8
COLS = 64
PIX = ROWS * COLS
EXT = PIX + 2 * COLS
CH = 512
HALF = 256
TOK = 128
PIECE = 16
STEP = 128


def dot(a, b):
    return jnp.dot(a, b, preferred_element_type=F32)


def dot_nt(a, b):
    return lax.dot_general(a, b, (((1,), (1,)), ((), ())), preferred_element_type=F32)


def dot_tn(a, b):
    return lax.dot_general(a, b, (((0,), (0,)), ((), ())), preferred_element_type=F32)


def silu_gate(lifted):
    return 1.0 / (1.0 + jnp.exp(-lifted))


def shifted_columns(wide, store):
    col = lax.rem(lax.broadcasted_iota(jnp.int32, wide.shape, 0), COLS)
    down = pltpu.roll(wide, 1, 0)
    up = pltpu.roll(wide, wide.shape[0] - 1, 0)
    store(0, jnp.where(col == 0, 0.0, down).astype(BF16))
    store(1, wide.astype(BF16))
    store(2, jnp.where(col == COLS - 1, 0.0, up).astype(BF16))


def block_rows(tap):
    pieces = []
    row = tap * CH
    while row < (tap + 1) * CH:
        block, inside = divmod(row, 72)
        count = min(72 - inside, (tap + 1) * CH - row)
        pieces.append((block, inside, row - tap * CH, count))
        row += count
    return pieces


def place_of(half, block):
    x, z, y = block // 16, (block // 4) % 4, block % 4
    u, v = (x, y) if half == 0 else (y, x)
    return (z // 2) * 32 + u * 8 + v * 2 + z % 2


def whole_place(half, block):
    x, z, y = block // 16, (block // 4) % 4, block % 4
    u, v = (x, y) if half == 0 else (y, x)
    return u * 16 + v * 4 + z


def kernel(
    lengths,
    pix_in,
    hid_in,
    enc_in,
    attn_in,
    time_in,
    wq_in,
    wk_in,
    wv_in,
    wo_in,
    wt_in,
    wc_in,
    cot_in,
    res_out,
    gconv_out,
    gout_out,
    pix,
    cot,
    hid_own,
    hid,
    wq,
    wk,
    wv,
    wo,
    wt,
    wc,
    kv,
    film,
    normed,
    query,
    att,
    mix,
    act3,
    cot3,
    gact_send,
    gact_recv,
    gact_own,
    gmix,
    result,
    cv,
    core_send,
    core_recv,
    s1,
    r1,
    a1,
    s2,
    r2,
    a2,
    s3,
    r3,
    ov,
    core_send_o,
    core_recv_o,
    s1o,
    r1o,
    a1o,
    s2o,
    r2o,
    a2o,
    s3o,
    r3o,
    a3o,
    out_peer,
    load_sem,
    send_sem,
    recv_sem,
):
    x = lax.axis_index("dp_0")
    z = lax.axis_index("dp_1")
    y = lax.axis_index("space_0")
    core = lax.axis_index("space_1")
    chan = lax.axis_index("chan")
    other = 1 - chan
    slab = y * 2 + core
    piece = x * 2 + core
    count = [0]

    def remote(src, dst, device):
        i = count[0]
        count[0] += 1
        return pltpu.make_async_remote_copy(
            src_ref=src,
            dst_ref=dst,
            send_sem=send_sem.at[i],
            recv_sem=recv_sem.at[i],
            device_id=device,
            device_id_type=MESH,
        )

    def slab_device(d):
        s = lax.rem(slab + d, 8)
        return {"space_0": s // 2, "space_1": lax.rem(s, 2)}

    u = x * (1 - core) + y * core
    v = y * (1 - core) + x * core

    def first_device(d):
        t = lax.rem(u + d, 4)
        return {"dp_0": t * (1 - core) + x * core, "space_0": y * (1 - core) + t * core}

    def second_device(d):
        t = lax.rem(v + d, 4)
        return {"dp_0": x * (1 - core) + t * core, "space_0": t * (1 - core) + y * core}

    def depth_core_device(d, k):
        return {"dp_1": lax.rem(z + d, 4), "space_1": k}

    def depth_device(d):
        return {"dp_1": lax.rem(z + d, 4)}

    peer_chan = {"chan": other}
    peer_core = {"space_1": 1 - core}
    half_x, low_x = x // 2, lax.rem(x, 2)
    dest = [{"dp_0": 2 * chan + low_x, "space_1": k, "chan": 1 - half_x} for k in range(2)]
    source = [{"dp_0": 2 * (1 - chan) + low_x, "space_1": k, "chan": half_x} for k in range(2)]

    def piece_device(d):
        p = lax.rem(piece + d, 8)
        return {"dp_0": p // 2, "space_1": lax.rem(p, 2)}

    barrier = pltpu.get_barrier_semaphore()
    greeted = (
        [peer_chan]
        + dest
        + source
        + [depth_device(d) for d in range(1, 4)]
        + [depth_core_device(d, 1 - core) for d in range(1, 4)]
        + [piece_device(d) for d in range(1, 8)]
        + [slab_device(d) for d in range(1, 8)]
    )
    for device in greeted:
        pl.semaphore_signal(barrier, inc=1, device_id=device, device_id_type=MESH)

    loads = []

    def load(src, dst):
        copy = pltpu.make_async_copy(src, dst, load_sem.at[len(loads)])
        copy.start()
        loads.append(copy)
        return copy

    ld_hid = load(hid_in, hid_own)
    ld_pix = load(pix_in, pix.at[COLS : COLS + PIX, :])
    ld_wq = load(wq_in, wq.at[chan])
    ld_cot = load(cot_in, cot.at[COLS : COLS + PIX, :])
    ld_wc = load(wc_in, wc)
    ld_wk = load(wk_in, wk)
    ld_wv = load(wv_in, wv)
    ld_wo = load(wo_in, wo.at[chan])
    ld_wt = load(wt_in, wt)

    top = (slab > 0).astype(F32)
    bottom = (slab < 7).astype(F32)
    attn = attn_in[...].astype(F32)
    attn_row = jnp.concatenate([attn[i : i + 1, :] for i in range(4)], axis=1)

    def query_rows(rows):
        part = pix[rows, :].astype(F32)
        mean = jnp.sum(part * part, axis=-1, keepdims=True) / 512.0
        norm = (part * lax.rsqrt(mean + 1e-06) * attn_row).astype(BF16)
        normed[rows, :] = norm
        query[chan, rows, :] = dot(norm, wq[chan]).astype(BF16)

    ld_pix.wait()
    ld_wq.wait()

    @pl.loop(0, PIX // STEP)
    def _(m):
        query_rows(pl.ds(pl.multiple_of(m * STEP + COLS, COLS), STEP))

    ld_hid.wait()
    ld_cot.wait()
    pl.semaphore_wait(barrier, len(greeted))

    hid_copies = []
    for d in range(1, 8):
        s = lax.rem(slab + d, 8)
        there = pl.ds(pl.multiple_of(s * PIECE, PIECE), PIECE)
        hid_copies.append(remote(hid_own.at[there, :], hid.at[slab], slab_device(d)))
        hid_copies[-1].start()
    wq_rows = pl.ds(pl.multiple_of(piece * 64, 64), 64)
    wo_rows = pl.ds(pl.multiple_of(piece * 32, 32), 32)
    w_copies = [
        remote(wq_in.at[wq_rows, :], wq.at[chan, wq_rows, :], peer_chan),
        remote(wo_in.at[wo_rows, :], wo.at[chan, wo_rows, :], peer_chan),
    ]
    for copy in w_copies:
        copy.start()
    halos = [
        remote(pix.at[PIX : PIX + COLS, :], pix.at[0:COLS, :], slab_device(1)),
        remote(pix.at[COLS : 2 * COLS, :], pix.at[COLS + PIX : EXT, :], slab_device(7)),
        remote(cot.at[PIX : PIX + COLS, :], cot.at[0:COLS, :], slab_device(1)),
        remote(cot.at[COLS : 2 * COLS, :], cot.at[COLS + PIX : EXT, :], slab_device(7)),
    ]
    for copy in halos:
        copy.start()

    def shift_cot(start, size, factor):
        wide = cot[start : start + size, :].astype(F32)
        if factor is not None:
            wide = wide * factor

        def put_cot(b, value):
            cot3[b, start : start + size, :] = value

        shifted_columns(wide, put_cot)

    shift_cot(COLS, PIX, None)
    ld_wc.wait()

    def grad_half(which, m):
        total = None
        for a in range(3):
            for b in range(3):
                tap = 3 * a + b
                left = cot3[2 - b, pl.ds(pl.multiple_of((2 - a) * COLS + m * STEP, COLS), STEP), :]
                rows = pl.ds(pl.multiple_of(tap * CH + which * HALF, HALF), HALF)
                term = dot_nt(left, wc[rows, :])
                total = term if total is None else total + term
        return total

    def grad_rows(m):
        rows = pl.ds(pl.multiple_of(m * STEP, STEP), STEP)
        gact_send[rows, :] = grad_half(other, m).astype(BF16)
        gact_own[rows, :] = grad_half(chan, m)

    @pl.loop(1, 3)
    def _(m):
        grad_rows(m)

    gact_inner = remote(
        gact_send.at[STEP : 3 * STEP, :], gact_recv.at[STEP : 3 * STEP, :], peer_chan
    )

    enc = enc_in[...].astype(F32)
    ld_wk.wait()
    ld_wv.wait()
    for copy in hid_copies:
        copy.wait()
    own_tokens = pl.ds(pl.multiple_of(slab * PIECE, PIECE), PIECE)
    hid[slab] = hid_own[own_tokens, :]
    squares = None
    for s in range(8):
        part = hid[s].astype(F32)
        part = jnp.sum(part * part, axis=-1, keepdims=True)
        squares = part if squares is None else squares + part
    scale = lax.rsqrt(squares / 4096.0 + 1e-06)
    key_sum, value_sum = None, None
    for s in range(8):
        gain = jnp.concatenate([enc[4 * s + i : 4 * s + i + 1, :] for i in range(4)], axis=1)
        context = (hid[s].astype(F32) * scale * gain).astype(BF16)
        key_part = dot(context, wk[s * CH : (s + 1) * CH, :])
        value_part = dot(context, wv[s * CH : (s + 1) * CH, :])
        key_sum = key_part if key_sum is None else key_sum + key_part
        value_sum = value_part if value_sum is None else value_sum + value_part
    kv[chan, own_tokens, 0:HALF] = key_sum.astype(BF16)
    kv[chan, own_tokens, HALF:CH] = value_sum.astype(BF16)
    kv_cross = remote(kv.at[chan, own_tokens, :], kv.at[chan, own_tokens, :], peer_chan)
    kv_cross.start()
    kv_copies = []
    for d in range(1, 8):
        kv_copies.append(
            remote(kv.at[chan, own_tokens, :], kv.at[chan, own_tokens, :], slab_device(d))
        )
        kv_copies[-1].start()
    gact_inner.start()

    w_spread = []
    for copy in w_copies:
        copy.wait()
    for d in range(1, 8):
        w_spread.append(
            remote(wq.at[other, wq_rows, :], wq.at[other, wq_rows, :], piece_device(d))
        )
        w_spread[-1].start()
    for d in range(1, 8):
        w_spread.append(
            remote(wo.at[other, wo_rows, :], wo.at[other, wo_rows, :], piece_device(d))
        )
        w_spread[-1].start()

    for copy in halos:
        copy.wait()
    query_rows(pl.ds(0, COLS))
    query_rows(pl.ds(COLS + PIX, COLS))
    shift_cot(0, COLS, top)
    shift_cot(COLS + PIX, COLS, bottom)

    @pl.loop(0, 2)
    def _(m):
        grad_rows(m * 3)

    gact_edges = [
        remote(gact_send.at[at : at + STEP, :], gact_recv.at[at : at + STEP, :], peer_chan)
        for at in (0, 3 * STEP)
    ]
    for copy in gact_edges:
        copy.start()

    kv_cross.wait()
    kv_spread = []
    for d in range(1, 8):
        kv_spread.append(
            remote(kv.at[other, own_tokens, :], kv.at[other, own_tokens, :], slab_device(d))
        )
        kv_spread[-1].start()

    ld_wt.wait()
    time_row = jnp.broadcast_to(time_in[...].astype(F32), (16, CH)).astype(BF16)
    film_rows = dot(time_row, wt[...])
    for h in range(2):
        film[h, 0] = film_rows[0:8, h * HALF : (h + 1) * HALF]
        film[h, 1] = film_rows[0:8, CH + h * HALF : CH + (h + 1) * HALF]

    ld_wo.wait()
    for copy in kv_copies:
        copy.wait()
    lane = lax.broadcasted_iota(jnp.int32, (TOK, STEP), 1)
    low_lanes = lane < 64
    live = lax.broadcasted_iota(jnp.int32, (STEP, TOK), 1) < lengths[0]
    zero = jnp.zeros((TOK, STEP), BF16)

    def attend(group, rows):
        for pair in range(2):
            at = pair * STEP
            keys = kv[group, :, at : at + STEP]
            values = kv[group, :, HALF + at : HALF + at + STEP]
            total = None
            for head in range(2):
                keep = low_lanes if head == 0 else jnp.logical_not(low_lanes)
                scores = dot_nt(query[group, rows, at : at + STEP], jnp.where(keep, keys, zero))
                scores = jnp.where(live, scores * 0.125, -1e30)
                peak = jnp.max(scores, axis=-1, keepdims=True)
                raised = jnp.exp(scores - peak)
                soft = raised / jnp.sum(raised, axis=-1, keepdims=True)
                term = dot(soft.astype(BF16), jnp.where(keep, values, zero))
                total = term if total is None else total + term
            att[group, rows, at : at + STEP] = total.astype(BF16)

    @pl.loop(0, EXT // STEP)
    def _(m):
        rows = pl.ds(pl.multiple_of(m * STEP, STEP), STEP)
        attend(chan, rows)
        mixed = pix[rows, :].astype(F32) + dot(att[chan, rows, :], wo[chan])
        mix[0, rows, :] = mixed[:, 0:HALF]
        mix[1, rows, :] = mixed[:, HALF:CH]

    for copy in w_spread[:7]:
        copy.wait()

    @pl.loop(0, EXT // STEP)
    def _(m):
        rows = pl.ds(pl.multiple_of(m * STEP, STEP), STEP)
        query[other, rows, :] = dot(normed[rows, :], wq[other]).astype(BF16)

    for copy in kv_spread:
        copy.wait()
    for copy in w_spread[7:]:
        copy.wait()

    @pl.loop(0, EXT // STEP)
    def _(m):
        rows = pl.ds(pl.multiple_of(m * STEP, STEP), STEP)
        attend(other, rows)
        mixed = dot(att[other, rows, :], wo[other])
        mix[0, rows, :] += mixed[:, 0:HALF]
        mix[1, rows, :] += mixed[:, HALF:CH]

    for h in range(2):
        lifted = mix[h] * (1.0 + film[h, 0, 0:1, :]) + film[h, 1, 0:1, :]
        active = lifted * silu_gate(lifted)
        active = jnp.concatenate(
            [active[0:COLS] * top, active[COLS : COLS + PIX], active[COLS + PIX : EXT] * bottom],
            axis=0,
        )

        def put_act(b, value):
            act3[b, :, h * HALF : (h + 1) * HALF] = value

        shifted_columns(active.astype(BF16).astype(F32), put_act)

    for tap in range(9):
        a, b = divmod(tap, 3)
        term = dot_tn(act3[b, a * COLS : a * COLS + PIX, :], cot[COLS : COLS + PIX, :])
        for block, inside, row, size in block_rows(tap):
            for h in range(2):
                at = place_of(h, block) * 72 + inside
                cv[h, at : at + size, :] = term[row : row + size, h * STEP : (h + 1) * STEP]

    to_core = []
    for c in range(2):

        @pl.loop(0, 2304 // 144)
        def _(i):
            rows = pl.ds(pl.multiple_of(c * 2304 + i * 144, 16), 144)
            core_send[rows, :] = cv[1 - core, rows, :].astype(BF16)

        rows = slice(c * 2304, (c + 1) * 2304)
        to_core.append(remote(core_send.at[rows, :], core_recv.at[rows, :], peer_core))
        to_core[-1].start()

    gact_inner.wait()
    for copy in gact_edges:
        copy.wait()

    @pl.loop(0, PIX // STEP)
    def _(m):
        rows = pl.ds(pl.multiple_of(m * STEP, STEP), STEP)
        rows_ext = pl.ds(pl.multiple_of(m * STEP + COLS, COLS), STEP)
        gain = 1.0 + film[chan, 0, 0:1, :]
        lifted = mix[chan, rows_ext, :] * gain + film[chan, 1, 0:1, :]
        gate = silu_gate(lifted)
        grad_act = gact_own[rows, :] + gact_recv[rows, :].astype(F32)
        grad_lift = grad_act * gate * (1.0 + lifted * (1.0 - gate))
        gmix[rows, :] = (cot[rows_ext, :].astype(F32) + grad_lift * gain).astype(BF16)

    first = [[], []]

    def first_stage(c):
        to_core[c].wait()
        for d in range(1, 4):
            start = c * 2304 + lax.rem(u + d, 4) * 576

            @pl.loop(0, 4)
            def _(i):
                rows = pl.ds(pl.multiple_of(start + i * 144, 16), 144)
                total = cv[core, rows, :] + core_recv[rows, :].astype(F32)
                s1[c, d - 1, pl.ds(pl.multiple_of(i * 144, 16), 144), :] = total.astype(BF16)

            first[c].append(remote(s1.at[c, d - 1], r1.at[c, d - 1], first_device(d)))
            first[c][-1].start()

    first_stage(0)

    for to in range(2):
        term = dot_tn(gmix[...], att[to, COLS : COLS + PIX, :])
        for low in range(2):
            for zz in range(4):
                for yy in range(4):
                    row = low * 128 + zz * 32 + yy * 8
                    block = (2 * (1 - to) + low) * 16 + zz * 4 + yy
                    for h in range(2):
                        at = whole_place(h, block) * 8
                        ov[h, at : at + 8, :] = term[row : row + 8, h * STEP : (h + 1) * STEP]
    core_send_o[...] = ov[1 - core].astype(BF16)
    to_core_o = remote(core_send_o, core_recv_o, peer_core)
    to_core_o.start()

    to_core_o.wait()
    first_o = []
    for d in range(1, 4):
        rows = pl.ds(pl.multiple_of(lax.rem(u + d, 4) * 128, 128), 128)
        total = ov[core, rows, :] + core_recv_o[rows, :].astype(F32)
        s1o[d - 1] = total.astype(BF16)
        first_o.append(remote(s1o.at[d - 1], r1o.at[d - 1], first_device(d)))
        first_o[-1].start()
    first_stage(1)

    @pl.loop(0, PIX // STEP)
    def _(m):
        rows = pl.ds(pl.multiple_of(m * STEP, STEP), STEP)
        rows_ext = pl.ds(pl.multiple_of(m * STEP + COLS, COLS), STEP)
        total = mix[chan, rows_ext, :]
        for a in range(3):
            for b in range(3):
                tap = 3 * a + b
                left = act3[b, pl.ds(pl.multiple_of(a * COLS + m * STEP, COLS), STEP), :]
                total = total + dot(left, wc[tap * CH : (tap + 1) * CH, :])
        result[rows, :] = total.astype(BF16)

    put_result = pltpu.make_async_copy(result, res_out, load_sem.at[len(loads)])
    put_result.start()

    for c in range(2):

        @pl.loop(0, 4)
        def _(i):
            rows = pl.ds(pl.multiple_of(c * 2304 + u * 576 + i * 144, 16), 144)
            a1[c, pl.ds(pl.multiple_of(i * 144, 16), 144), :] = cv[core, rows, :] + core_recv[
                rows, :
            ].astype(F32)

    for copy in first_o:
        copy.wait()
    rows = pl.ds(pl.multiple_of(u * 128, 128), 128)
    a1o[...] = (
        ov[core, rows, :]
        + core_recv_o[rows, :].astype(F32)
        + r1o[0].astype(F32)
        + r1o[1].astype(F32)
        + r1o[2].astype(F32)
    )
    second_o = []
    for d in range(1, 4):
        rows = pl.ds(pl.multiple_of(lax.rem(v + d, 4) * 32, 32), 32)
        s2o[d - 1] = a1o[rows, :].astype(BF16)
        second_o.append(remote(s2o.at[d - 1], r2o.at[d - 1], second_device(d)))
        second_o[-1].start()

    second = [[], []]

    def second_total(c, at):
        rows = pl.ds(pl.multiple_of(at * 144, 16), 144)
        return (
            a1[c, rows, :]
            + r1[c, 0, rows, :].astype(F32)
            + r1[c, 1, rows, :].astype(F32)
            + r1[c, 2, rows, :].astype(F32)
        )

    def second_stage(c):
        for copy in first[c]:
            copy.wait()
        for d in range(1, 4):
            s2[c, d - 1] = second_total(c, lax.rem(v + d, 4)).astype(BF16)
            second[c].append(remote(s2.at[c, d - 1], r2.at[c, d - 1], second_device(d)))
            second[c][-1].start()

    second_stage(0)
    a2[0] = second_total(0, v)
    for copy in second_o:
        copy.wait()
    rows = pl.ds(pl.multiple_of(v * 32, 32), 32)
    a2o[...] = (
        a1o[rows, :] + r2o[0].astype(F32) + r2o[1].astype(F32) + r2o[2].astype(F32)
    )
    third_o = []
    for d in range(1, 4):
        rows = pl.ds(pl.multiple_of(lax.rem(z + d, 4) * 8, 8), 8)
        s3o[d - 1] = a2o[rows, :]
        third_o.append(remote(s3o.at[d - 1], r3o.at[d - 1], depth_device(d)))
        third_o[-1].start()
    second_stage(1)
    a2[1] = second_total(1, v)
    for copy in third_o:
        copy.wait()
    rows = pl.ds(pl.multiple_of(z * 8, 8), 8)
    a3o[...] = a2o[rows, :] + r3o[0] + r3o[1] + r3o[2]
    last = []
    base = count[0]
    count[0] += 2
    for k in range(2):
        last.append(
            pltpu.make_async_remote_copy(
                src_ref=a3o,
                dst_ref=out_peer.at[core],
                send_sem=send_sem.at[base + k],
                recv_sem=recv_sem.at[base + core],
                device_id=dest[k],
                device_id_type=MESH,
            )
        )
        last[-1].start()

    for c in range(2):
        for copy in second[c]:
            copy.wait()
        a2[c] = (
            a2[c] + r2[c, 0].astype(F32) + r2[c, 1].astype(F32) + r2[c, 2].astype(F32)
        )

    def third_rows(t, k):
        rows = pl.ds(pl.multiple_of(lax.rem(t, 2) * 72, 8), 72)
        total = a2[t // 2, rows, :]
        return jnp.where(k == 0, total[0:36], total[36:72])

    pad = jnp.zeros((12, STEP), F32)
    third = []
    for d in range(8):
        step, swap = d // 2, d % 2
        if d == 0:
            continue
        k = 1 - core if swap else core
        total = third_rows(lax.rem(z + step, 4), k)
        s3[d - 1] = jnp.concatenate([total, pad], axis=0).astype(BF16)
        third.append(remote(s3.at[d - 1], r3.at[d - 1], depth_core_device(step, k)))
        third[-1].start()
    own = third_rows(z, core)
    first_core = core == 0
    for copy in third:
        copy.wait()
    mine = own + r3[1].astype(F32)[0:36] + r3[3].astype(F32)[0:36] + r3[5].astype(F32)[0:36]
    cross = (
        r3[0].astype(F32) + r3[2].astype(F32) + r3[4].astype(F32) + r3[6].astype(F32)
    )[0:36]
    gconv_out[:, 0:STEP] = jnp.where(first_core, mine, cross)
    gconv_out[:, STEP:HALF] = jnp.where(first_core, cross, mine)
    for copy in last:
        copy.wait_send()
    for k in range(2):
        pltpu.make_async_remote_copy(
            src_ref=a3o,
            dst_ref=out_peer.at[k],
            send_sem=send_sem.at[base + k],
            recv_sem=recv_sem.at[base + k],
            device_id=source[k],
            device_id_type=MESH,
        ).wait_recv()
        gout_out[:, k * STEP : (k + 1) * STEP] = jnp.where(
            first_core, out_peer[k, 0:4], out_peer[k, 4:8]
        )
    put_result.wait()
    assert count[0] == COPIES


def output_kernel(a, b, c, a_out, b_out, c_out, sems):
    copies = [
        pltpu.make_async_copy(src, dst, sems.at[i])
        for i, (src, dst) in enumerate(((a, a_out), (b, b_out), (c, c_out)))
    ]
    for copy in copies:
        copy.start()
    for copy in copies:
        copy.wait()


COPIES = 78
VMEM = pltpu.VMEM
ANY = pl.BlockSpec(memory_space=pl.ANY)
INSIDE = pl.BlockSpec(memory_space=pltpu.VMEM)


def time_embed(time_steps, emb_width):
    half_width = emb_width // 2
    lane = jnp.arange(emb_width)
    place = lax.rem(lane, half_width).astype(F32)
    frequency = jnp.exp(-math.log(10000.0) * place / half_width)
    angles = time_steps.astype(F32)[:, None] * frequency[None, :]
    return jnp.where((lane < half_width)[None, :], jnp.sin(angles), jnp.cos(angles)).astype(BF16)


def shards(
    pixels,
    hidden,
    enc_gain,
    lengths,
    time_steps,
    attn_gain,
    w_query,
    w_key,
    w_value,
    w_out,
    w_time,
    w_conv,
    cotangent,
):
    time_row = time_embed(time_steps, TEMB)
    result, grad_conv, grad_out_t = pl.pallas_call(
        kernel,
        out_shape=(
            jax.ShapeDtypeStruct((PIX, HALF), BF16),
            jax.ShapeDtypeStruct((36, HALF), F32),
            jax.ShapeDtypeStruct((4, HALF), F32),
        ),
        in_specs=[
            pl.BlockSpec(memory_space=pltpu.SMEM),
            ANY,
            ANY,
            INSIDE,
            INSIDE,
            INSIDE,
            ANY,
            ANY,
            ANY,
            ANY,
            ANY,
            ANY,
            ANY,
        ],
        out_specs=(ANY, INSIDE, INSIDE),
        scratch_shapes=[
            VMEM((EXT, CH), BF16),
            VMEM((EXT, HALF), BF16),
            VMEM((TOK, CH), BF16),
            VMEM((8, PIECE, CH), BF16),
            VMEM((2, CH, HALF), BF16),
            VMEM((4096, HALF), BF16),
            VMEM((4096, HALF), BF16),
            VMEM((2, HALF, CH), BF16),
            VMEM((TEMB, 2 * CH), BF16),
            VMEM((9 * CH, HALF), BF16),
            VMEM((2, TOK, CH), BF16),
            VMEM((2, 2, 8, HALF), F32),
            VMEM((EXT, CH), BF16),
            VMEM((2, EXT, HALF), BF16),
            VMEM((2, EXT, HALF), BF16),
            VMEM((2, EXT, HALF), F32),
            VMEM((3, EXT, CH), BF16),
            VMEM((3, EXT, HALF), BF16),
            VMEM((PIX, HALF), BF16),
            VMEM((PIX, HALF), BF16),
            VMEM((PIX, HALF), F32),
            VMEM((PIX, HALF), BF16),
            VMEM((PIX, HALF), BF16),
            VMEM((2, 4608, STEP), F32),
            VMEM((4608, STEP), BF16),
            VMEM((4608, STEP), BF16),
            VMEM((2, 3, 576, STEP), BF16),
            VMEM((2, 3, 576, STEP), BF16),
            VMEM((2, 576, STEP), F32),
            VMEM((2, 3, 144, STEP), BF16),
            VMEM((2, 3, 144, STEP), BF16),
            VMEM((2, 144, STEP), F32),
            VMEM((7, 48, STEP), BF16),
            VMEM((7, 48, STEP), BF16),
            VMEM((2, 512, STEP), F32),
            VMEM((512, STEP), BF16),
            VMEM((512, STEP), BF16),
            VMEM((3, 128, STEP), BF16),
            VMEM((3, 128, STEP), BF16),
            VMEM((128, STEP), F32),
            VMEM((3, 32, STEP), BF16),
            VMEM((3, 32, STEP), BF16),
            VMEM((32, STEP), F32),
            VMEM((3, 8, STEP), F32),
            VMEM((3, 8, STEP), F32),
            VMEM((8, STEP), F32),
            VMEM((2, 8, STEP), F32),
            pltpu.SemaphoreType.DMA((10,)),
            pltpu.SemaphoreType.DMA((COPIES,)),
            pltpu.SemaphoreType.DMA((COPIES,)),
        ],
        compiler_params=pltpu.CompilerParams(
            collective_id=0, has_side_effects=True, vmem_limit_bytes=60 * 1024 * 1024
        ),
        name="block",
    )(
        lengths,
        pixels.reshape(PIX, CH),
        hidden.reshape(TOK, CH),
        enc_gain.reshape(32, STEP),
        attn_gain.reshape(4, STEP),
        time_row,
        w_query,
        w_key,
        w_value,
        w_out,
        w_time,
        w_conv,
        cotangent.reshape(PIX, HALF),
    )
    result, grad_conv, grad_out_t = pl.pallas_call(
        output_kernel,
        out_shape=(
            jax.ShapeDtypeStruct((PIX, HALF), BF16),
            jax.ShapeDtypeStruct((36, HALF), F32),
            jax.ShapeDtypeStruct((4, HALF), F32),
        ),
        in_specs=[ANY] * 3,
        out_specs=(INSIDE,) * 3,
        scratch_shapes=[pltpu.SemaphoreType.DMA((3,))],
        compiler_params=pltpu.CompilerParams(vmem_limit_bytes=60 * 1024 * 1024),
        name="outputs",
    )(result, grad_conv, grad_out_t)
    return result.reshape(1, ROWS, COLS, HALF), grad_conv, grad_out_t


def solution(mesh):
    finer = Mesh(
        mesh.devices.reshape(4, 4, 4, 2, mesh.shape["chan"]),
        ("dp_0", "dp_1", "space_0", "space_1", "chan"),
    )
    placed = (
        P(DP, SPACE, None, None),
        P(DP, None, SPACE),
        P(),
        P(DP),
        P(DP),
        P(),
        P(None, "chan"),
        P(None, "chan"),
        P(None, "chan"),
        P("chan", None),
        P(),
        P(None, "chan"),
        P(DP, SPACE, None, "chan"),
    )
    return jax.shard_map(
        shards,
        mesh=finer,
        in_specs=placed,
        out_specs=(P(DP, SPACE, None, "chan"), P(DP_SPACE, "chan"), P(DP_SPACE, "chan")),
        check_vma=False,
    )
```

```python
import math

import jax
import jax.numpy as jnp
from jax import lax
from jax.experimental import pallas as pl
from jax.experimental.pallas import tpu as pltpu
from jax.sharding import Mesh
from jax.sharding import PartitionSpec as P

TEMB = 512
SPACE = ("space_0", "space_1")
DP_SPACE = ("dp_0", "dp_1", "space_0", "space_1")
DP = ("dp_0", "dp_1")
F32 = jnp.float32
BF16 = jnp.bfloat16
MESH = pl.DeviceIdType.MESH

ROWS = 8
COLS = 64
PIX = ROWS * COLS
EXT = PIX + 2 * COLS
CH = 512
HALF = 256
TOK = 128
PIECE = 16
STEP = 128
WIDE = 320


def dot(a, b):
    return jnp.dot(a, b, preferred_element_type=F32)


def dot_nt(a, b):
    return lax.dot_general(a, b, (((1,), (1,)), ((), ())), preferred_element_type=F32)


def dot_tn(a, b):
    return lax.dot_general(a, b, (((0,), (0,)), ((), ())), preferred_element_type=F32)


def silu_gate(lifted):
    return 1.0 / (1.0 + jnp.exp(-lifted))


def shifted_columns(wide, store):
    col = lax.rem(lax.broadcasted_iota(jnp.int32, wide.shape, 0), COLS)
    down = pltpu.roll(wide, 1, 0)
    up = pltpu.roll(wide, wide.shape[0] - 1, 0)
    store(0, jnp.where(col == 0, 0.0, down).astype(BF16))
    store(1, wide.astype(BF16))
    store(2, jnp.where(col == COLS - 1, 0.0, up).astype(BF16))


def block_rows(tap):
    pieces = []
    row = tap * CH
    while row < (tap + 1) * CH:
        block, inside = divmod(row, 72)
        count = min(72 - inside, (tap + 1) * CH - row)
        pieces.append((block, inside, row - tap * CH, count))
        row += count
    return pieces


def place_of(half, block):
    x, z, y = block // 16, (block // 4) % 4, block % 4
    u, v = (x, y) if half == 0 else (y, x)
    return (z // 2) * 32 + u * 8 + v * 2 + z % 2


def whole_place(half, block):
    x, z, y = block // 16, (block // 4) % 4, block % 4
    u, v = (x, y) if half == 0 else (y, x)
    return u * 16 + v * 4 + z


def kernel(
    lengths,
    pix_in,
    hid_in,
    enc_in,
    attn_in,
    time_in,
    wq_in,
    wk_in,
    wv_in,
    wo_in,
    wt_in,
    wc_in,
    cot_in,
    res_out,
    gconv_out,
    gout_out,
    pix,
    cot,
    hid_own,
    hid,
    wq,
    wk,
    wv,
    wo,
    wt,
    wc,
    kv,
    film,
    normed,
    query,
    att,
    mix,
    act3,
    cot3,
    gact_send,
    gact_recv,
    gact_own,
    gmix,
    result,
    cv,
    core_send,
    core_recv,
    s1,
    r1,
    a1,
    s2,
    r2,
    a2,
    s3,
    r3,
    ov,
    core_send_o,
    core_recv_o,
    s1o,
    r1o,
    a1o,
    s2o,
    r2o,
    a2o,
    s3o,
    r3o,
    a3o,
    out_peer,
    load_sem,
    send_sem,
    recv_sem,
):
    x = lax.axis_index("dp_0")
    z = lax.axis_index("dp_1")
    y = lax.axis_index("space_0")
    core = lax.axis_index("space_1")
    chan = lax.axis_index("chan")
    other = 1 - chan
    slab = y * 2 + core
    piece = x * 2 + core
    count = [0]

    def remote(src, dst, device):
        i = count[0]
        count[0] += 1
        return pltpu.make_async_remote_copy(
            src_ref=src,
            dst_ref=dst,
            send_sem=send_sem.at[i],
            recv_sem=recv_sem.at[i],
            device_id=device,
            device_id_type=MESH,
        )

    def slab_device(d):
        s = lax.rem(slab + d, 8)
        return {"space_0": s // 2, "space_1": lax.rem(s, 2)}

    u = x * (1 - core) + y * core
    v = y * (1 - core) + x * core

    def first_device(d):
        t = lax.rem(u + d, 4)
        return {"dp_0": t * (1 - core) + x * core, "space_0": y * (1 - core) + t * core}

    def second_device(d):
        t = lax.rem(v + d, 4)
        return {"dp_0": x * (1 - core) + t * core, "space_0": t * (1 - core) + y * core}

    def depth_core_device(d, k):
        return {"dp_1": lax.rem(z + d, 4), "space_1": k}

    def depth_device(d):
        return {"dp_1": lax.rem(z + d, 4)}

    peer_chan = {"chan": other}
    peer_core = {"space_1": 1 - core}
    half_x, low_x = x // 2, lax.rem(x, 2)
    dest = [{"dp_0": 2 * chan + low_x, "space_1": k, "chan": 1 - half_x} for k in range(2)]
    source = [{"dp_0": 2 * (1 - chan) + low_x, "space_1": k, "chan": half_x} for k in range(2)]

    def piece_device(d):
        p = lax.rem(piece + d, 8)
        return {"dp_0": p // 2, "space_1": lax.rem(p, 2)}

    barrier = pltpu.get_barrier_semaphore()
    greeted = (
        [peer_chan]
        + dest
        + source
        + [depth_device(d) for d in range(1, 4)]
        + [depth_core_device(d, 1 - core) for d in range(1, 4)]
        + [piece_device(d) for d in range(1, 8)]
        + [slab_device(d) for d in range(1, 8)]
    )
    for device in greeted:
        pl.semaphore_signal(barrier, inc=1, device_id=device, device_id_type=MESH)

    loads = []

    def load(src, dst):
        copy = pltpu.make_async_copy(src, dst, load_sem.at[len(loads)])
        copy.start()
        loads.append(copy)
        return copy

    ld_hid = load(hid_in, hid_own)
    ld_pix = load(pix_in, pix.at[COLS : COLS + PIX, :])
    ld_wq = load(wq_in, wq.at[chan])
    ld_cot = load(cot_in, cot.at[COLS : COLS + PIX, :])
    ld_wc = load(wc_in, wc)
    ld_wk = load(wk_in, wk)
    ld_wv = load(wv_in, wv)
    ld_wo = load(wo_in, wo.at[chan])
    ld_wt = load(wt_in, wt)

    top = (slab > 0).astype(F32)
    bottom = (slab < 7).astype(F32)
    attn = attn_in[...].astype(F32)
    attn_row = jnp.concatenate([attn[i : i + 1, :] for i in range(4)], axis=1)

    def query_rows(rows):
        part = pix[rows, :].astype(F32)
        mean = jnp.sum(part * part, axis=-1, keepdims=True) / 512.0
        norm = (part * lax.rsqrt(mean + 1e-06) * attn_row).astype(BF16)
        normed[rows, :] = norm
        query[chan, rows, :] = dot(norm, wq[chan]).astype(BF16)

    ld_pix.wait()
    ld_wq.wait()

    @pl.loop(0, PIX // STEP)
    def _(m):
        query_rows(pl.ds(pl.multiple_of(m * STEP + COLS, COLS), STEP))

    ld_hid.wait()
    ld_cot.wait()
    pl.semaphore_wait(barrier, len(greeted))

    hid_copies = []
    for d in range(1, 8):
        s = lax.rem(slab + d, 8)
        there = pl.ds(pl.multiple_of(s * PIECE, PIECE), PIECE)
        hid_copies.append(remote(hid_own.at[there, :], hid.at[slab], slab_device(d)))
        hid_copies[-1].start()
    wq_rows = pl.ds(pl.multiple_of(piece * 64, 64), 64)
    wo_rows = pl.ds(pl.multiple_of(piece * 32, 32), 32)
    w_copies = [
        remote(wq_in.at[wq_rows, :], wq.at[chan, wq_rows, :], peer_chan),
        remote(wo_in.at[wo_rows, :], wo.at[chan, wo_rows, :], peer_chan),
    ]
    for copy in w_copies:
        copy.start()
    halos = [
        remote(pix.at[PIX : PIX + COLS, :], pix.at[0:COLS, :], slab_device(1)),
        remote(pix.at[COLS : 2 * COLS, :], pix.at[COLS + PIX : EXT, :], slab_device(7)),
        remote(cot.at[PIX : PIX + COLS, :], cot.at[0:COLS, :], slab_device(1)),
        remote(cot.at[COLS : 2 * COLS, :], cot.at[COLS + PIX : EXT, :], slab_device(7)),
    ]
    for copy in halos:
        copy.start()

    def shift_cot(start, size, factor):
        wide = cot[start : start + size, :].astype(F32)
        if factor is not None:
            wide = wide * factor

        def put_cot(b, value):
            cot3[b, start : start + size, :] = value

        shifted_columns(wide, put_cot)

    shift_cot(COLS, PIX, None)
    ld_wc.wait()

    def grad_half(which, m):
        total = None
        for a in range(3):
            for b in range(3):
                tap = 3 * a + b
                left = cot3[2 - b, pl.ds(pl.multiple_of((2 - a) * COLS + m * STEP, COLS), STEP), :]
                rows = pl.ds(pl.multiple_of(tap * CH + which * HALF, HALF), HALF)
                term = dot_nt(left, wc[rows, :])
                total = term if total is None else total + term
        return total

    def grad_rows(m):
        rows = pl.ds(pl.multiple_of(m * STEP, STEP), STEP)
        gact_send[rows, :] = grad_half(other, m).astype(BF16)
        gact_own[rows, :] = grad_half(chan, m)

    @pl.loop(1, 3)
    def _(m):
        grad_rows(m)

    gact_inner = remote(
        gact_send.at[STEP : 3 * STEP, :], gact_recv.at[STEP : 3 * STEP, :], peer_chan
    )

    enc = enc_in[...].astype(F32)
    ld_wk.wait()
    ld_wv.wait()
    for copy in hid_copies:
        copy.wait()
    own_tokens = pl.ds(pl.multiple_of(slab * PIECE, PIECE), PIECE)
    hid[slab] = hid_own[own_tokens, :]
    squares = None
    for s in range(8):
        part = hid[s].astype(F32)
        part = jnp.sum(part * part, axis=-1, keepdims=True)
        squares = part if squares is None else squares + part
    scale = lax.rsqrt(squares / 4096.0 + 1e-06)
    key_sum, value_sum = None, None
    for s in range(8):
        gain = jnp.concatenate([enc[4 * s + i : 4 * s + i + 1, :] for i in range(4)], axis=1)
        context = (hid[s].astype(F32) * scale * gain).astype(BF16)
        key_part = dot(context, wk[s * CH : (s + 1) * CH, :])
        value_part = dot(context, wv[s * CH : (s + 1) * CH, :])
        key_sum = key_part if key_sum is None else key_sum + key_part
        value_sum = value_part if value_sum is None else value_sum + value_part
    kv[chan, own_tokens, 0:HALF] = key_sum.astype(BF16)
    kv[chan, own_tokens, HALF:CH] = value_sum.astype(BF16)
    kv_cross = remote(kv.at[chan, own_tokens, :], kv.at[chan, own_tokens, :], peer_chan)
    kv_cross.start()
    kv_copies = []
    for d in range(1, 8):
        kv_copies.append(
            remote(kv.at[chan, own_tokens, :], kv.at[chan, own_tokens, :], slab_device(d))
        )
        kv_copies[-1].start()
    gact_inner.start()

    w_spread = []
    for copy in w_copies:
        copy.wait()
    for d in range(1, 8):
        w_spread.append(
            remote(wq.at[other, wq_rows, :], wq.at[other, wq_rows, :], piece_device(d))
        )
        w_spread[-1].start()
    for d in range(1, 8):
        w_spread.append(
            remote(wo.at[other, wo_rows, :], wo.at[other, wo_rows, :], piece_device(d))
        )
        w_spread[-1].start()

    for copy in halos:
        copy.wait()
    query_rows(pl.ds(0, COLS))
    query_rows(pl.ds(COLS + PIX, COLS))
    shift_cot(0, COLS, top)
    shift_cot(COLS + PIX, COLS, bottom)

    @pl.loop(0, 2)
    def _(m):
        grad_rows(m * 3)

    gact_edges = [
        remote(gact_send.at[at : at + STEP, :], gact_recv.at[at : at + STEP, :], peer_chan)
        for at in (0, 3 * STEP)
    ]
    for copy in gact_edges:
        copy.start()

    kv_cross.wait()
    kv_spread = []
    for d in range(1, 8):
        kv_spread.append(
            remote(kv.at[other, own_tokens, :], kv.at[other, own_tokens, :], slab_device(d))
        )
        kv_spread[-1].start()

    ld_wt.wait()
    time_row = jnp.broadcast_to(time_in[...].astype(F32), (16, CH)).astype(BF16)
    film_rows = dot(time_row, wt[...])
    for h in range(2):
        film[h, 0] = film_rows[0:8, h * HALF : (h + 1) * HALF]
        film[h, 1] = film_rows[0:8, CH + h * HALF : CH + (h + 1) * HALF]

    ld_wo.wait()
    for copy in kv_copies:
        copy.wait()
    lane = lax.broadcasted_iota(jnp.int32, (TOK, STEP), 1)
    low_lanes = lane < 64
    live = lax.broadcasted_iota(jnp.int32, (WIDE, TOK), 1) < lengths[0]
    zero = jnp.zeros((TOK, STEP), BF16)

    def attend(group, rows):
        for pair in range(2):
            at = pair * STEP
            keys = kv[group, :, at : at + STEP]
            values = kv[group, :, HALF + at : HALF + at + STEP]
            total = None
            for head in range(2):
                keep = low_lanes if head == 0 else jnp.logical_not(low_lanes)
                scores = dot_nt(query[group, rows, at : at + STEP], jnp.where(keep, keys, zero))
                scores = jnp.where(live, scores * 0.125, -1e30)
                peak = jnp.max(scores, axis=-1, keepdims=True)
                raised = jnp.exp(scores - peak)
                soft = raised * (1.0 / jnp.sum(raised, axis=-1, keepdims=True))
                term = dot(soft.astype(BF16), jnp.where(keep, values, zero))
                total = term if total is None else total + term
            att[group, rows, at : at + STEP] = total.astype(BF16)

    @pl.loop(0, EXT // WIDE)
    def _(m):
        rows = pl.ds(pl.multiple_of(m * WIDE, COLS), WIDE)
        attend(chan, rows)
        mixed = pix[rows, :].astype(F32) + dot(att[chan, rows, :], wo[chan])
        mix[0, rows, :] = mixed[:, 0:HALF]
        mix[1, rows, :] = mixed[:, HALF:CH]

    for copy in w_spread[:7]:
        copy.wait()

    @pl.loop(0, EXT // STEP)
    def _(m):
        rows = pl.ds(pl.multiple_of(m * STEP, STEP), STEP)
        query[other, rows, :] = dot(normed[rows, :], wq[other]).astype(BF16)

    for copy in kv_spread:
        copy.wait()
    for copy in w_spread[7:]:
        copy.wait()

    @pl.loop(0, EXT // WIDE)
    def _(m):
        rows = pl.ds(pl.multiple_of(m * WIDE, COLS), WIDE)
        attend(other, rows)
        mixed = dot(att[other, rows, :], wo[other])
        mix[0, rows, :] += mixed[:, 0:HALF]
        mix[1, rows, :] += mixed[:, HALF:CH]

    for h in range(2):
        lifted = mix[h] * (1.0 + film[h, 0, 0:1, :]) + film[h, 1, 0:1, :]
        active = lifted * silu_gate(lifted)
        active = jnp.concatenate(
            [active[0:COLS] * top, active[COLS : COLS + PIX], active[COLS + PIX : EXT] * bottom],
            axis=0,
        )

        def put_act(b, value):
            act3[b, :, h * HALF : (h + 1) * HALF] = value

        shifted_columns(active.astype(BF16).astype(F32), put_act)

    for tap in range(9):
        a, b = divmod(tap, 3)
        term = dot_tn(act3[b, a * COLS : a * COLS + PIX, :], cot[COLS : COLS + PIX, :])
        for block, inside, row, size in block_rows(tap):
            for h in range(2):
                at = place_of(h, block) * 72 + inside
                cv[h, at : at + size, :] = term[row : row + size, h * STEP : (h + 1) * STEP]

    to_core = []
    for c in range(2):

        @pl.loop(0, 2304 // 144)
        def _(i):
            rows = pl.ds(pl.multiple_of(c * 2304 + i * 144, 16), 144)
            core_send[rows, :] = cv[1 - core, rows, :].astype(BF16)

        rows = slice(c * 2304, (c + 1) * 2304)
        to_core.append(remote(core_send.at[rows, :], core_recv.at[rows, :], peer_core))
        to_core[-1].start()

    gact_inner.wait()
    for copy in gact_edges:
        copy.wait()

    @pl.loop(0, PIX // STEP)
    def _(m):
        rows = pl.ds(pl.multiple_of(m * STEP, STEP), STEP)
        rows_ext = pl.ds(pl.multiple_of(m * STEP + COLS, COLS), STEP)
        gain = 1.0 + film[chan, 0, 0:1, :]
        lifted = mix[chan, rows_ext, :] * gain + film[chan, 1, 0:1, :]
        gate = silu_gate(lifted)
        grad_act = gact_own[rows, :] + gact_recv[rows, :].astype(F32)
        grad_lift = grad_act * gate * (1.0 + lifted * (1.0 - gate))
        gmix[rows, :] = (cot[rows_ext, :].astype(F32) + grad_lift * gain).astype(BF16)

    first = [[], []]

    def first_stage(c):
        to_core[c].wait()
        for d in range(1, 4):
            start = c * 2304 + lax.rem(u + d, 4) * 576

            @pl.loop(0, 4)
            def _(i):
                rows = pl.ds(pl.multiple_of(start + i * 144, 16), 144)
                total = cv[core, rows, :] + core_recv[rows, :].astype(F32)
                s1[c, d - 1, pl.ds(pl.multiple_of(i * 144, 16), 144), :] = total.astype(BF16)

            first[c].append(remote(s1.at[c, d - 1], r1.at[c, d - 1], first_device(d)))
            first[c][-1].start()

    first_stage(0)

    for to in range(2):
        term = dot_tn(gmix[...], att[to, COLS : COLS + PIX, :])
        for low in range(2):
            for zz in range(4):
                for yy in range(4):
                    row = low * 128 + zz * 32 + yy * 8
                    block = (2 * (1 - to) + low) * 16 + zz * 4 + yy
                    for h in range(2):
                        at = whole_place(h, block) * 8
                        ov[h, at : at + 8, :] = term[row : row + 8, h * STEP : (h + 1) * STEP]
    core_send_o[...] = ov[1 - core].astype(BF16)
    to_core_o = remote(core_send_o, core_recv_o, peer_core)
    to_core_o.start()

    to_core_o.wait()
    first_o = []
    for d in range(1, 4):
        rows = pl.ds(pl.multiple_of(lax.rem(u + d, 4) * 128, 128), 128)
        total = ov[core, rows, :] + core_recv_o[rows, :].astype(F32)
        s1o[d - 1] = total.astype(BF16)
        first_o.append(remote(s1o.at[d - 1], r1o.at[d - 1], first_device(d)))
        first_o[-1].start()
    first_stage(1)

    @pl.loop(0, PIX // STEP)
    def _(m):
        rows = pl.ds(pl.multiple_of(m * STEP, STEP), STEP)
        rows_ext = pl.ds(pl.multiple_of(m * STEP + COLS, COLS), STEP)
        total = mix[chan, rows_ext, :]
        for a in range(3):
            for b in range(3):
                tap = 3 * a + b
                left = act3[b, pl.ds(pl.multiple_of(a * COLS + m * STEP, COLS), STEP), :]
                total = total + dot(left, wc[tap * CH : (tap + 1) * CH, :])
        result[rows, :] = total.astype(BF16)

    put_result = pltpu.make_async_copy(result, res_out, load_sem.at[len(loads)])
    put_result.start()

    for c in range(2):

        @pl.loop(0, 4)
        def _(i):
            rows = pl.ds(pl.multiple_of(c * 2304 + u * 576 + i * 144, 16), 144)
            a1[c, pl.ds(pl.multiple_of(i * 144, 16), 144), :] = cv[core, rows, :] + core_recv[
                rows, :
            ].astype(F32)

    for copy in first_o:
        copy.wait()
    rows = pl.ds(pl.multiple_of(u * 128, 128), 128)
    a1o[...] = (
        ov[core, rows, :]
        + core_recv_o[rows, :].astype(F32)
        + r1o[0].astype(F32)
        + r1o[1].astype(F32)
        + r1o[2].astype(F32)
    )
    second_o = []
    for d in range(1, 4):
        rows = pl.ds(pl.multiple_of(lax.rem(v + d, 4) * 32, 32), 32)
        s2o[d - 1] = a1o[rows, :].astype(BF16)
        second_o.append(remote(s2o.at[d - 1], r2o.at[d - 1], second_device(d)))
        second_o[-1].start()

    second = [[], []]

    def second_total(c, at):
        rows = pl.ds(pl.multiple_of(at * 144, 16), 144)
        return (
            a1[c, rows, :]
            + r1[c, 0, rows, :].astype(F32)
            + r1[c, 1, rows, :].astype(F32)
            + r1[c, 2, rows, :].astype(F32)
        )

    def second_stage(c):
        for copy in first[c]:
            copy.wait()
        for d in range(1, 4):
            s2[c, d - 1] = second_total(c, lax.rem(v + d, 4)).astype(BF16)
            second[c].append(remote(s2.at[c, d - 1], r2.at[c, d - 1], second_device(d)))
            second[c][-1].start()

    second_stage(0)
    a2[0] = second_total(0, v)
    for copy in second_o:
        copy.wait()
    rows = pl.ds(pl.multiple_of(v * 32, 32), 32)
    a2o[...] = (
        a1o[rows, :] + r2o[0].astype(F32) + r2o[1].astype(F32) + r2o[2].astype(F32)
    )
    third_o = []
    for d in range(1, 4):
        rows = pl.ds(pl.multiple_of(lax.rem(z + d, 4) * 8, 8), 8)
        s3o[d - 1] = a2o[rows, :]
        third_o.append(remote(s3o.at[d - 1], r3o.at[d - 1], depth_device(d)))
        third_o[-1].start()
    second_stage(1)
    a2[1] = second_total(1, v)
    for copy in third_o:
        copy.wait()
    rows = pl.ds(pl.multiple_of(z * 8, 8), 8)
    a3o[...] = a2o[rows, :] + r3o[0] + r3o[1] + r3o[2]
    last = []
    base = count[0]
    count[0] += 2
    for k in range(2):
        last.append(
            pltpu.make_async_remote_copy(
                src_ref=a3o,
                dst_ref=out_peer.at[core],
                send_sem=send_sem.at[base + k],
                recv_sem=recv_sem.at[base + core],
                device_id=dest[k],
                device_id_type=MESH,
            )
        )
        last[-1].start()

    for c in range(2):
        for copy in second[c]:
            copy.wait()
        a2[c] = (
            a2[c] + r2[c, 0].astype(F32) + r2[c, 1].astype(F32) + r2[c, 2].astype(F32)
        )

    def third_rows(t, k):
        rows = pl.ds(pl.multiple_of(lax.rem(t, 2) * 72, 8), 72)
        total = a2[t // 2, rows, :]
        return jnp.where(k == 0, total[0:36], total[36:72])

    pad = jnp.zeros((12, STEP), F32)
    third = []
    for d in range(8):
        step, swap = d // 2, d % 2
        if d == 0:
            continue
        k = 1 - core if swap else core
        total = third_rows(lax.rem(z + step, 4), k)
        s3[d - 1] = jnp.concatenate([total, pad], axis=0).astype(BF16)
        third.append(remote(s3.at[d - 1], r3.at[d - 1], depth_core_device(step, k)))
        third[-1].start()
    own = third_rows(z, core)
    first_core = core == 0
    for copy in third:
        copy.wait()
    mine = own + r3[1].astype(F32)[0:36] + r3[3].astype(F32)[0:36] + r3[5].astype(F32)[0:36]
    cross = (
        r3[0].astype(F32) + r3[2].astype(F32) + r3[4].astype(F32) + r3[6].astype(F32)
    )[0:36]
    gconv_out[:, 0:STEP] = jnp.where(first_core, mine, cross)
    gconv_out[:, STEP:HALF] = jnp.where(first_core, cross, mine)
    for copy in last:
        copy.wait_send()
    for k in range(2):
        pltpu.make_async_remote_copy(
            src_ref=a3o,
            dst_ref=out_peer.at[k],
            send_sem=send_sem.at[base + k],
            recv_sem=recv_sem.at[base + k],
            device_id=source[k],
            device_id_type=MESH,
        ).wait_recv()
        gout_out[:, k * STEP : (k + 1) * STEP] = jnp.where(
            first_core, out_peer[k, 0:4], out_peer[k, 4:8]
        )
    put_result.wait()
    assert count[0] == COPIES


def output_kernel(a, b, c, a_out, b_out, c_out, sems):
    copies = [
        pltpu.make_async_copy(src, dst, sems.at[i])
        for i, (src, dst) in enumerate(((a, a_out), (b, b_out), (c, c_out)))
    ]
    for copy in copies:
        copy.start()
    for copy in copies:
        copy.wait()


COPIES = 78
VMEM = pltpu.VMEM
ANY = pl.BlockSpec(memory_space=pl.ANY)
INSIDE = pl.BlockSpec(memory_space=pltpu.VMEM)


def time_embed(time_steps, emb_width):
    half_width = emb_width // 2
    lane = jnp.arange(emb_width)
    place = lax.rem(lane, half_width).astype(F32)
    frequency = jnp.exp(-math.log(10000.0) * place / half_width)
    angles = time_steps.astype(F32)[:, None] * frequency[None, :]
    return jnp.where((lane < half_width)[None, :], jnp.sin(angles), jnp.cos(angles)).astype(BF16)


def shards(
    pixels,
    hidden,
    enc_gain,
    lengths,
    time_steps,
    attn_gain,
    w_query,
    w_key,
    w_value,
    w_out,
    w_time,
    w_conv,
    cotangent,
):
    time_row = time_embed(time_steps, TEMB)
    result, grad_conv, grad_out_t = pl.pallas_call(
        kernel,
        out_shape=(
            jax.ShapeDtypeStruct((PIX, HALF), BF16),
            jax.ShapeDtypeStruct((36, HALF), F32),
            jax.ShapeDtypeStruct((4, HALF), F32),
        ),
        in_specs=[
            pl.BlockSpec(memory_space=pltpu.SMEM),
            ANY,
            ANY,
            INSIDE,
            INSIDE,
            INSIDE,
            ANY,
            ANY,
            ANY,
            ANY,
            ANY,
            ANY,
            ANY,
        ],
        out_specs=(ANY, INSIDE, INSIDE),
        scratch_shapes=[
            VMEM((EXT, CH), BF16),
            VMEM((EXT, HALF), BF16),
            VMEM((TOK, CH), BF16),
            VMEM((8, PIECE, CH), BF16),
            VMEM((2, CH, HALF), BF16),
            VMEM((4096, HALF), BF16),
            VMEM((4096, HALF), BF16),
            VMEM((2, HALF, CH), BF16),
            VMEM((TEMB, 2 * CH), BF16),
            VMEM((9 * CH, HALF), BF16),
            VMEM((2, TOK, CH), BF16),
            VMEM((2, 2, 8, HALF), F32),
            VMEM((EXT, CH), BF16),
            VMEM((2, EXT, HALF), BF16),
            VMEM((2, EXT, HALF), BF16),
            VMEM((2, EXT, HALF), F32),
            VMEM((3, EXT, CH), BF16),
            VMEM((3, EXT, HALF), BF16),
            VMEM((PIX, HALF), BF16),
            VMEM((PIX, HALF), BF16),
            VMEM((PIX, HALF), F32),
            VMEM((PIX, HALF), BF16),
            VMEM((PIX, HALF), BF16),
            VMEM((2, 4608, STEP), F32),
            VMEM((4608, STEP), BF16),
            VMEM((4608, STEP), BF16),
            VMEM((2, 3, 576, STEP), BF16),
            VMEM((2, 3, 576, STEP), BF16),
            VMEM((2, 576, STEP), F32),
            VMEM((2, 3, 144, STEP), BF16),
            VMEM((2, 3, 144, STEP), BF16),
            VMEM((2, 144, STEP), F32),
            VMEM((7, 48, STEP), BF16),
            VMEM((7, 48, STEP), BF16),
            VMEM((2, 512, STEP), F32),
            VMEM((512, STEP), BF16),
            VMEM((512, STEP), BF16),
            VMEM((3, 128, STEP), BF16),
            VMEM((3, 128, STEP), BF16),
            VMEM((128, STEP), F32),
            VMEM((3, 32, STEP), BF16),
            VMEM((3, 32, STEP), BF16),
            VMEM((32, STEP), F32),
            VMEM((3, 8, STEP), F32),
            VMEM((3, 8, STEP), F32),
            VMEM((8, STEP), F32),
            VMEM((2, 8, STEP), F32),
            pltpu.SemaphoreType.DMA((10,)),
            pltpu.SemaphoreType.DMA((COPIES,)),
            pltpu.SemaphoreType.DMA((COPIES,)),
        ],
        compiler_params=pltpu.CompilerParams(
            collective_id=0, has_side_effects=True, vmem_limit_bytes=60 * 1024 * 1024
        ),
        name="block",
    )(
        lengths,
        pixels.reshape(PIX, CH),
        hidden.reshape(TOK, CH),
        enc_gain.reshape(32, STEP),
        attn_gain.reshape(4, STEP),
        time_row,
        w_query,
        w_key,
        w_value,
        w_out,
        w_time,
        w_conv,
        cotangent.reshape(PIX, HALF),
    )
    result, grad_conv, grad_out_t = pl.pallas_call(
        output_kernel,
        out_shape=(
            jax.ShapeDtypeStruct((PIX, HALF), BF16),
            jax.ShapeDtypeStruct((36, HALF), F32),
            jax.ShapeDtypeStruct((4, HALF), F32),
        ),
        in_specs=[ANY] * 3,
        out_specs=(INSIDE,) * 3,
        scratch_shapes=[pltpu.SemaphoreType.DMA((3,))],
        compiler_params=pltpu.CompilerParams(vmem_limit_bytes=60 * 1024 * 1024),
        name="outputs",
    )(result, grad_conv, grad_out_t)
    return result.reshape(1, ROWS, COLS, HALF), grad_conv, grad_out_t


def solution(mesh):
    finer = Mesh(
        mesh.devices.reshape(4, 4, 4, 2, mesh.shape["chan"]),
        ("dp_0", "dp_1", "space_0", "space_1", "chan"),
    )
    placed = (
        P(DP, SPACE, None, None),
        P(DP, None, SPACE),
        P(),
        P(DP),
        P(DP),
        P(),
        P(None, "chan"),
        P(None, "chan"),
        P(None, "chan"),
        P("chan", None),
        P(),
        P(None, "chan"),
        P(DP, SPACE, None, "chan"),
    )
    return jax.shard_map(
        shards,
        mesh=finer,
        in_specs=placed,
        out_specs=(P(DP, SPACE, None, "chan"), P(DP_SPACE, "chan"), P(DP_SPACE, "chan")),
        check_vma=False,
    )
```

```python
import math

import jax
import jax.numpy as jnp
from jax import lax
from jax.experimental import pallas as pl
from jax.experimental.pallas import tpu as pltpu
from jax.sharding import Mesh
from jax.sharding import PartitionSpec as P

TEMB = 512
SPACE = ("space_0", "space_1")
DP_SPACE = ("dp_0", "dp_1", "space_0", "space_1")
DP = ("dp_0", "dp_1")
F32 = jnp.float32
BF16 = jnp.bfloat16
MESH = pl.DeviceIdType.MESH

ROWS = 8
COLS = 64
PIX = ROWS * COLS
EXT = PIX + 2 * COLS
CH = 512
HALF = 256
TOK = 128
PIECE = 16
STEP = 128
WIDE = 640
GATE = 256


def dot(a, b):
    return jnp.dot(a, b, preferred_element_type=F32)


def dot_nt(a, b):
    return lax.dot_general(a, b, (((1,), (1,)), ((), ())), preferred_element_type=F32)


def dot_tn(a, b):
    return lax.dot_general(a, b, (((0,), (0,)), ((), ())), preferred_element_type=F32)


def silu_gate(lifted):
    return 1.0 / (1.0 + jnp.exp(-lifted))


def shifted_columns(wide, store):
    col = lax.rem(lax.broadcasted_iota(jnp.int32, wide.shape, 0), COLS)
    down = pltpu.roll(wide, 1, 0)
    up = pltpu.roll(wide, wide.shape[0] - 1, 0)
    store(0, jnp.where(col == 0, 0.0, down).astype(BF16))
    store(1, wide.astype(BF16))
    store(2, jnp.where(col == COLS - 1, 0.0, up).astype(BF16))


def block_rows(tap):
    pieces = []
    row = tap * CH
    while row < (tap + 1) * CH:
        block, inside = divmod(row, 72)
        count = min(72 - inside, (tap + 1) * CH - row)
        pieces.append((block, inside, row - tap * CH, count))
        row += count
    return pieces


def place_of(half, block):
    x, z, y = block // 16, (block // 4) % 4, block % 4
    u, v = (x, y) if half == 0 else (y, x)
    return (z // 2) * 32 + u * 8 + v * 2 + z % 2


def whole_place(half, block):
    x, z, y = block // 16, (block // 4) % 4, block % 4
    u, v = (x, y) if half == 0 else (y, x)
    return u * 16 + v * 4 + z


def kernel(
    lengths,
    pix_in,
    hid_in,
    enc_in,
    attn_in,
    time_in,
    wq_in,
    wk_in,
    wv_in,
    wo_in,
    wt_in,
    wc_in,
    cot_in,
    res_out,
    gconv_out,
    gout_out,
    pix,
    cot,
    hid_own,
    hid,
    wq,
    wk,
    wv,
    wo,
    wt,
    wc,
    kv,
    film,
    normed,
    query,
    att,
    mix,
    act3,
    cot3,
    gact_send,
    gact_recv,
    gact_own,
    gmix,
    result,
    cv,
    core_send,
    core_recv,
    s1,
    r1,
    a1,
    s2,
    r2,
    a2,
    s3,
    r3,
    ov,
    core_send_o,
    core_recv_o,
    s1o,
    r1o,
    a1o,
    s2o,
    r2o,
    a2o,
    s3o,
    r3o,
    a3o,
    out_peer,
    load_sem,
    send_sem,
    recv_sem,
):
    x = lax.axis_index("dp_0")
    z = lax.axis_index("dp_1")
    y = lax.axis_index("space_0")
    core = lax.axis_index("space_1")
    chan = lax.axis_index("chan")
    other = 1 - chan
    slab = y * 2 + core
    piece = x * 2 + core
    count = [0]

    def remote(src, dst, device):
        i = count[0]
        count[0] += 1
        return pltpu.make_async_remote_copy(
            src_ref=src,
            dst_ref=dst,
            send_sem=send_sem.at[i],
            recv_sem=recv_sem.at[i],
            device_id=device,
            device_id_type=MESH,
        )

    def slab_device(d):
        s = lax.rem(slab + d, 8)
        return {"space_0": s // 2, "space_1": lax.rem(s, 2)}

    u = x * (1 - core) + y * core
    v = y * (1 - core) + x * core

    def first_device(d):
        t = lax.rem(u + d, 4)
        return {"dp_0": t * (1 - core) + x * core, "space_0": y * (1 - core) + t * core}

    def second_device(d):
        t = lax.rem(v + d, 4)
        return {"dp_0": x * (1 - core) + t * core, "space_0": t * (1 - core) + y * core}

    def depth_core_device(d, k):
        return {"dp_1": lax.rem(z + d, 4), "space_1": k}

    def depth_device(d):
        return {"dp_1": lax.rem(z + d, 4)}

    peer_chan = {"chan": other}
    peer_core = {"space_1": 1 - core}
    half_x, low_x = x // 2, lax.rem(x, 2)
    dest = [{"dp_0": 2 * chan + low_x, "space_1": k, "chan": 1 - half_x} for k in range(2)]
    source = [{"dp_0": 2 * (1 - chan) + low_x, "space_1": k, "chan": half_x} for k in range(2)]

    def piece_device(d):
        p = lax.rem(piece + d, 8)
        return {"dp_0": p // 2, "space_1": lax.rem(p, 2)}

    barrier = pltpu.get_barrier_semaphore()
    greeted = (
        [peer_chan]
        + dest
        + source
        + [depth_device(d) for d in range(1, 4)]
        + [depth_core_device(d, 1 - core) for d in range(1, 4)]
        + [piece_device(d) for d in range(1, 8)]
        + [slab_device(d) for d in range(1, 8)]
    )
    for device in greeted:
        pl.semaphore_signal(barrier, inc=1, device_id=device, device_id_type=MESH)

    loads = []

    def load(src, dst):
        copy = pltpu.make_async_copy(src, dst, load_sem.at[len(loads)])
        copy.start()
        loads.append(copy)
        return copy

    ld_hid = load(hid_in, hid_own)
    ld_pix = load(pix_in, pix.at[COLS : COLS + PIX, :])
    ld_wq = load(wq_in, wq.at[chan])
    ld_cot = load(cot_in, cot.at[COLS : COLS + PIX, :])
    ld_wc = load(wc_in, wc)
    ld_wk = load(wk_in, wk)
    ld_wv = load(wv_in, wv)
    ld_wo = load(wo_in, wo.at[chan])
    ld_wt = load(wt_in, wt)

    top = (slab > 0).astype(F32)
    bottom = (slab < 7).astype(F32)
    attn = attn_in[...].astype(F32)
    attn_row = jnp.concatenate([attn[i : i + 1, :] for i in range(4)], axis=1)

    def query_rows(rows):
        part = pix[rows, :].astype(F32)
        mean = jnp.sum(part * part, axis=-1, keepdims=True) / 512.0
        norm = (part * lax.rsqrt(mean + 1e-06) * attn_row).astype(BF16)
        normed[rows, :] = norm
        query[chan, rows, :] = dot(norm, wq[chan]).astype(BF16)

    ld_pix.wait()
    ld_wq.wait()

    @pl.loop(0, PIX // STEP)
    def _(m):
        query_rows(pl.ds(pl.multiple_of(m * STEP + COLS, COLS), STEP))

    ld_hid.wait()
    ld_cot.wait()
    pl.semaphore_wait(barrier, len(greeted))

    hid_copies = []
    for d in range(1, 8):
        s = lax.rem(slab + d, 8)
        there = pl.ds(pl.multiple_of(s * PIECE, PIECE), PIECE)
        hid_copies.append(remote(hid_own.at[there, :], hid.at[slab], slab_device(d)))
        hid_copies[-1].start()
    wq_rows = pl.ds(pl.multiple_of(piece * 64, 64), 64)
    wo_rows = pl.ds(pl.multiple_of(piece * 32, 32), 32)
    w_copies = [
        remote(wq_in.at[wq_rows, :], wq.at[chan, wq_rows, :], peer_chan),
        remote(wo_in.at[wo_rows, :], wo.at[chan, wo_rows, :], peer_chan),
    ]
    for copy in w_copies:
        copy.start()
    halos = [
        remote(pix.at[PIX : PIX + COLS, :], pix.at[0:COLS, :], slab_device(1)),
        remote(pix.at[COLS : 2 * COLS, :], pix.at[COLS + PIX : EXT, :], slab_device(7)),
        remote(cot.at[PIX : PIX + COLS, :], cot.at[0:COLS, :], slab_device(1)),
        remote(cot.at[COLS : 2 * COLS, :], cot.at[COLS + PIX : EXT, :], slab_device(7)),
    ]
    for copy in halos:
        copy.start()

    def shift_cot(start, size, factor):
        wide = cot[start : start + size, :].astype(F32)
        if factor is not None:
            wide = wide * factor

        def put_cot(b, value):
            cot3[b, start : start + size, :] = value

        shifted_columns(wide, put_cot)

    shift_cot(COLS, PIX, None)
    ld_wc.wait()

    def grad_half(which, m):
        total = None
        for a in range(3):
            for b in range(3):
                tap = 3 * a + b
                left = cot3[2 - b, pl.ds(pl.multiple_of((2 - a) * COLS + m * STEP, COLS), STEP), :]
                rows = pl.ds(pl.multiple_of(tap * CH + which * HALF, HALF), HALF)
                term = dot_nt(left, wc[rows, :])
                total = term if total is None else total + term
        return total

    def grad_rows(m):
        rows = pl.ds(pl.multiple_of(m * STEP, STEP), STEP)
        gact_send[rows, :] = grad_half(other, m).astype(BF16)
        gact_own[rows, :] = grad_half(chan, m)

    @pl.loop(1, 3)
    def _(m):
        grad_rows(m)

    gact_inner = remote(
        gact_send.at[STEP : 3 * STEP, :], gact_recv.at[STEP : 3 * STEP, :], peer_chan
    )

    enc = enc_in[...].astype(F32)
    ld_wk.wait()
    ld_wv.wait()
    for copy in hid_copies:
        copy.wait()
    own_tokens = pl.ds(pl.multiple_of(slab * PIECE, PIECE), PIECE)
    hid[slab] = hid_own[own_tokens, :]
    squares = None
    for s in range(8):
        part = hid[s].astype(F32)
        part = jnp.sum(part * part, axis=-1, keepdims=True)
        squares = part if squares is None else squares + part
    scale = lax.rsqrt(squares / 4096.0 + 1e-06)
    key_sum, value_sum = None, None
    for s in range(8):
        gain = jnp.concatenate([enc[4 * s + i : 4 * s + i + 1, :] for i in range(4)], axis=1)
        context = (hid[s].astype(F32) * scale * gain).astype(BF16)
        key_part = dot(context, wk[s * CH : (s + 1) * CH, :])
        value_part = dot(context, wv[s * CH : (s + 1) * CH, :])
        key_sum = key_part if key_sum is None else key_sum + key_part
        value_sum = value_part if value_sum is None else value_sum + value_part
    kv[chan, own_tokens, 0:HALF] = key_sum.astype(BF16)
    kv[chan, own_tokens, HALF:CH] = value_sum.astype(BF16)
    kv_cross = remote(kv.at[chan, own_tokens, :], kv.at[chan, own_tokens, :], peer_chan)
    kv_cross.start()
    kv_copies = []
    for d in range(1, 8):
        kv_copies.append(
            remote(kv.at[chan, own_tokens, :], kv.at[chan, own_tokens, :], slab_device(d))
        )
        kv_copies[-1].start()
    gact_inner.start()

    w_spread = []
    for copy in w_copies:
        copy.wait()
    for d in range(1, 8):
        w_spread.append(
            remote(wq.at[other, wq_rows, :], wq.at[other, wq_rows, :], piece_device(d))
        )
        w_spread[-1].start()
    for d in range(1, 8):
        w_spread.append(
            remote(wo.at[other, wo_rows, :], wo.at[other, wo_rows, :], piece_device(d))
        )
        w_spread[-1].start()

    for copy in halos:
        copy.wait()
    query_rows(pl.ds(0, COLS))
    query_rows(pl.ds(COLS + PIX, COLS))
    shift_cot(0, COLS, top)
    shift_cot(COLS + PIX, COLS, bottom)

    @pl.loop(0, 2)
    def _(m):
        grad_rows(m * 3)

    gact_edges = [
        remote(gact_send.at[at : at + STEP, :], gact_recv.at[at : at + STEP, :], peer_chan)
        for at in (0, 3 * STEP)
    ]
    for copy in gact_edges:
        copy.start()

    kv_cross.wait()
    kv_spread = []
    for d in range(1, 8):
        kv_spread.append(
            remote(kv.at[other, own_tokens, :], kv.at[other, own_tokens, :], slab_device(d))
        )
        kv_spread[-1].start()

    ld_wt.wait()
    time_row = jnp.broadcast_to(time_in[...].astype(F32), (16, CH)).astype(BF16)
    film_rows = dot(time_row, wt[...])
    for h in range(2):
        film[h, 0] = film_rows[0:8, h * HALF : (h + 1) * HALF]
        film[h, 1] = film_rows[0:8, CH + h * HALF : CH + (h + 1) * HALF]

    ld_wo.wait()
    for copy in kv_copies:
        copy.wait()
    lane = lax.broadcasted_iota(jnp.int32, (TOK, STEP), 1)
    low_lanes = lane < 64
    live = lax.broadcasted_iota(jnp.int32, (WIDE, TOK), 1) < lengths[0]
    zero = jnp.zeros((TOK, STEP), BF16)

    def attend(group, rows):
        for pair in range(2):
            at = pair * STEP
            keys = kv[group, :, at : at + STEP]
            values = kv[group, :, HALF + at : HALF + at + STEP]
            total = None
            for head in range(2):
                keep = low_lanes if head == 0 else jnp.logical_not(low_lanes)
                scores = dot_nt(query[group, rows, at : at + STEP], jnp.where(keep, keys, zero))
                scores = jnp.where(live, scores * 0.125, -1e30)
                peak = jnp.max(scores, axis=-1, keepdims=True)
                raised = jnp.exp(scores - peak)
                soft = raised * (1.0 / jnp.sum(raised, axis=-1, keepdims=True))
                term = dot(soft.astype(BF16), jnp.where(keep, values, zero))
                total = term if total is None else total + term
            att[group, rows, at : at + STEP] = total.astype(BF16)

    @pl.loop(0, EXT // WIDE)
    def _(m):
        rows = pl.ds(pl.multiple_of(m * WIDE, COLS), WIDE)
        attend(chan, rows)
        mixed = pix[rows, :].astype(F32) + dot(att[chan, rows, :], wo[chan])
        mix[0, rows, :] = mixed[:, 0:HALF]
        mix[1, rows, :] = mixed[:, HALF:CH]

    for copy in w_spread[:7]:
        copy.wait()

    @pl.loop(0, EXT // STEP)
    def _(m):
        rows = pl.ds(pl.multiple_of(m * STEP, STEP), STEP)
        query[other, rows, :] = dot(normed[rows, :], wq[other]).astype(BF16)

    for copy in kv_spread:
        copy.wait()
    for copy in w_spread[7:]:
        copy.wait()

    @pl.loop(0, EXT // WIDE)
    def _(m):
        rows = pl.ds(pl.multiple_of(m * WIDE, COLS), WIDE)
        attend(other, rows)
        mixed = dot(att[other, rows, :], wo[other])
        mix[0, rows, :] += mixed[:, 0:HALF]
        mix[1, rows, :] += mixed[:, HALF:CH]

    for h in range(2):
        lifted = mix[h] * (1.0 + film[h, 0, 0:1, :]) + film[h, 1, 0:1, :]
        active = lifted * silu_gate(lifted)
        active = jnp.concatenate(
            [active[0:COLS] * top, active[COLS : COLS + PIX], active[COLS + PIX : EXT] * bottom],
            axis=0,
        )

        def put_act(b, value):
            act3[b, :, h * HALF : (h + 1) * HALF] = value

        shifted_columns(active.astype(BF16).astype(F32), put_act)

    for tap in range(9):
        a, b = divmod(tap, 3)
        term = dot_tn(act3[b, a * COLS : a * COLS + PIX, :], cot[COLS : COLS + PIX, :])
        for block, inside, row, size in block_rows(tap):
            for h in range(2):
                at = place_of(h, block) * 72 + inside
                cv[h, at : at + size, :] = term[row : row + size, h * STEP : (h + 1) * STEP]

    to_core = []
    for c in range(2):

        @pl.loop(0, 2304 // 144)
        def _(i):
            rows = pl.ds(pl.multiple_of(c * 2304 + i * 144, 16), 144)
            core_send[rows, :] = cv[1 - core, rows, :].astype(BF16)

        rows = slice(c * 2304, (c + 1) * 2304)
        to_core.append(remote(core_send.at[rows, :], core_recv.at[rows, :], peer_core))
        to_core[-1].start()

    gact_inner.wait()
    for copy in gact_edges:
        copy.wait()

    @pl.loop(0, PIX // GATE)
    def _(m):
        rows = pl.ds(pl.multiple_of(m * GATE, GATE), GATE)
        rows_ext = pl.ds(pl.multiple_of(m * GATE + COLS, COLS), GATE)
        gain = 1.0 + film[chan, 0, 0:1, :]
        lifted = mix[chan, rows_ext, :] * gain + film[chan, 1, 0:1, :]
        gate = silu_gate(lifted)
        grad_act = gact_own[rows, :] + gact_recv[rows, :].astype(F32)
        grad_lift = grad_act * gate * (1.0 + lifted * (1.0 - gate))
        gmix[rows, :] = (cot[rows_ext, :].astype(F32) + grad_lift * gain).astype(BF16)

    first = [[], []]

    def first_stage(c):
        to_core[c].wait()
        for d in range(1, 4):
            start = c * 2304 + lax.rem(u + d, 4) * 576

            @pl.loop(0, 4)
            def _(i):
                rows = pl.ds(pl.multiple_of(start + i * 144, 16), 144)
                total = cv[core, rows, :] + core_recv[rows, :].astype(F32)
                s1[c, d - 1, pl.ds(pl.multiple_of(i * 144, 16), 144), :] = total.astype(BF16)

            first[c].append(remote(s1.at[c, d - 1], r1.at[c, d - 1], first_device(d)))
            first[c][-1].start()

    first_stage(0)

    for to in range(2):
        term = dot_tn(gmix[...], att[to, COLS : COLS + PIX, :])
        for low in range(2):
            for zz in range(4):
                for yy in range(4):
                    row = low * 128 + zz * 32 + yy * 8
                    block = (2 * (1 - to) + low) * 16 + zz * 4 + yy
                    for h in range(2):
                        at = whole_place(h, block) * 8
                        ov[h, at : at + 8, :] = term[row : row + 8, h * STEP : (h + 1) * STEP]
    core_send_o[...] = ov[1 - core].astype(BF16)
    to_core_o = remote(core_send_o, core_recv_o, peer_core)
    to_core_o.start()

    to_core_o.wait()
    first_o = []
    for d in range(1, 4):
        rows = pl.ds(pl.multiple_of(lax.rem(u + d, 4) * 128, 128), 128)
        total = ov[core, rows, :] + core_recv_o[rows, :].astype(F32)
        s1o[d - 1] = total.astype(BF16)
        first_o.append(remote(s1o.at[d - 1], r1o.at[d - 1], first_device(d)))
        first_o[-1].start()
    first_stage(1)

    @pl.loop(0, PIX // STEP)
    def _(m):
        rows = pl.ds(pl.multiple_of(m * STEP, STEP), STEP)
        rows_ext = pl.ds(pl.multiple_of(m * STEP + COLS, COLS), STEP)
        total = mix[chan, rows_ext, :]
        for a in range(3):
            for b in range(3):
                tap = 3 * a + b
                left = act3[b, pl.ds(pl.multiple_of(a * COLS + m * STEP, COLS), STEP), :]
                total = total + dot(left, wc[tap * CH : (tap + 1) * CH, :])
        result[rows, :] = total.astype(BF16)

    put_result = pltpu.make_async_copy(result, res_out, load_sem.at[len(loads)])
    put_result.start()

    for c in range(2):

        @pl.loop(0, 4)
        def _(i):
            rows = pl.ds(pl.multiple_of(c * 2304 + u * 576 + i * 144, 16), 144)
            a1[c, pl.ds(pl.multiple_of(i * 144, 16), 144), :] = cv[core, rows, :] + core_recv[
                rows, :
            ].astype(F32)

    for copy in first_o:
        copy.wait()
    rows = pl.ds(pl.multiple_of(u * 128, 128), 128)
    a1o[...] = (
        ov[core, rows, :]
        + core_recv_o[rows, :].astype(F32)
        + r1o[0].astype(F32)
        + r1o[1].astype(F32)
        + r1o[2].astype(F32)
    )
    second_o = []
    for d in range(1, 4):
        rows = pl.ds(pl.multiple_of(lax.rem(v + d, 4) * 32, 32), 32)
        s2o[d - 1] = a1o[rows, :].astype(BF16)
        second_o.append(remote(s2o.at[d - 1], r2o.at[d - 1], second_device(d)))
        second_o[-1].start()

    second = [[], []]

    def second_total(c, at):
        rows = pl.ds(pl.multiple_of(at * 144, 16), 144)
        return (
            a1[c, rows, :]
            + r1[c, 0, rows, :].astype(F32)
            + r1[c, 1, rows, :].astype(F32)
            + r1[c, 2, rows, :].astype(F32)
        )

    def second_stage(c):
        for copy in first[c]:
            copy.wait()
        for d in range(1, 4):
            s2[c, d - 1] = second_total(c, lax.rem(v + d, 4)).astype(BF16)
            second[c].append(remote(s2.at[c, d - 1], r2.at[c, d - 1], second_device(d)))
            second[c][-1].start()

    second_stage(0)
    a2[0] = second_total(0, v)
    for copy in second_o:
        copy.wait()
    rows = pl.ds(pl.multiple_of(v * 32, 32), 32)
    a2o[...] = (
        a1o[rows, :] + r2o[0].astype(F32) + r2o[1].astype(F32) + r2o[2].astype(F32)
    )
    third_o = []
    for d in range(1, 4):
        rows = pl.ds(pl.multiple_of(lax.rem(z + d, 4) * 8, 8), 8)
        s3o[d - 1] = a2o[rows, :]
        third_o.append(remote(s3o.at[d - 1], r3o.at[d - 1], depth_device(d)))
        third_o[-1].start()
    second_stage(1)
    a2[1] = second_total(1, v)
    for copy in third_o:
        copy.wait()
    rows = pl.ds(pl.multiple_of(z * 8, 8), 8)
    a3o[...] = a2o[rows, :] + r3o[0] + r3o[1] + r3o[2]
    last = []
    base = count[0]
    count[0] += 2
    for k in range(2):
        last.append(
            pltpu.make_async_remote_copy(
                src_ref=a3o,
                dst_ref=out_peer.at[core],
                send_sem=send_sem.at[base + k],
                recv_sem=recv_sem.at[base + core],
                device_id=dest[k],
                device_id_type=MESH,
            )
        )
        last[-1].start()

    for c in range(2):
        for copy in second[c]:
            copy.wait()
        a2[c] = (
            a2[c] + r2[c, 0].astype(F32) + r2[c, 1].astype(F32) + r2[c, 2].astype(F32)
        )

    def third_rows(t, k):
        rows = pl.ds(pl.multiple_of(lax.rem(t, 2) * 72, 8), 72)
        total = a2[t // 2, rows, :]
        return jnp.where(k == 0, total[0:36], total[36:72])

    pad = jnp.zeros((12, STEP), F32)
    third = []
    for d in range(8):
        step, swap = d // 2, d % 2
        if d == 0:
            continue
        k = 1 - core if swap else core
        total = third_rows(lax.rem(z + step, 4), k)
        s3[d - 1] = jnp.concatenate([total, pad], axis=0).astype(BF16)
        third.append(remote(s3.at[d - 1], r3.at[d - 1], depth_core_device(step, k)))
        third[-1].start()
    own = third_rows(z, core)
    first_core = core == 0
    for copy in third:
        copy.wait()
    mine = own + r3[1].astype(F32)[0:36] + r3[3].astype(F32)[0:36] + r3[5].astype(F32)[0:36]
    cross = (
        r3[0].astype(F32) + r3[2].astype(F32) + r3[4].astype(F32) + r3[6].astype(F32)
    )[0:36]
    gconv_out[:, 0:STEP] = jnp.where(first_core, mine, cross)
    gconv_out[:, STEP:HALF] = jnp.where(first_core, cross, mine)
    for copy in last:
        copy.wait_send()
    for k in range(2):
        pltpu.make_async_remote_copy(
            src_ref=a3o,
            dst_ref=out_peer.at[k],
            send_sem=send_sem.at[base + k],
            recv_sem=recv_sem.at[base + k],
            device_id=source[k],
            device_id_type=MESH,
        ).wait_recv()
        gout_out[:, k * STEP : (k + 1) * STEP] = jnp.where(
            first_core, out_peer[k, 0:4], out_peer[k, 4:8]
        )
    put_result.wait()
    assert count[0] == COPIES


def output_kernel(a, b, c, a_out, b_out, c_out, sems):
    copies = [
        pltpu.make_async_copy(src, dst, sems.at[i])
        for i, (src, dst) in enumerate(((a, a_out), (b, b_out), (c, c_out)))
    ]
    for copy in copies:
        copy.start()
    for copy in copies:
        copy.wait()


COPIES = 78
VMEM = pltpu.VMEM
ANY = pl.BlockSpec(memory_space=pl.ANY)
INSIDE = pl.BlockSpec(memory_space=pltpu.VMEM)


def time_embed(time_steps, emb_width):
    half_width = emb_width // 2
    lane = jnp.arange(emb_width)
    place = lax.rem(lane, half_width).astype(F32)
    frequency = jnp.exp(-math.log(10000.0) * place / half_width)
    angles = time_steps.astype(F32)[:, None] * frequency[None, :]
    return jnp.where((lane < half_width)[None, :], jnp.sin(angles), jnp.cos(angles)).astype(BF16)


def shards(
    pixels,
    hidden,
    enc_gain,
    lengths,
    time_steps,
    attn_gain,
    w_query,
    w_key,
    w_value,
    w_out,
    w_time,
    w_conv,
    cotangent,
):
    time_row = time_embed(time_steps, TEMB)
    result, grad_conv, grad_out_t = pl.pallas_call(
        kernel,
        out_shape=(
            jax.ShapeDtypeStruct((PIX, HALF), BF16),
            jax.ShapeDtypeStruct((36, HALF), F32),
            jax.ShapeDtypeStruct((4, HALF), F32),
        ),
        in_specs=[
            pl.BlockSpec(memory_space=pltpu.SMEM),
            ANY,
            ANY,
            INSIDE,
            INSIDE,
            INSIDE,
            ANY,
            ANY,
            ANY,
            ANY,
            ANY,
            ANY,
            ANY,
        ],
        out_specs=(ANY, INSIDE, INSIDE),
        scratch_shapes=[
            VMEM((EXT, CH), BF16),
            VMEM((EXT, HALF), BF16),
            VMEM((TOK, CH), BF16),
            VMEM((8, PIECE, CH), BF16),
            VMEM((2, CH, HALF), BF16),
            VMEM((4096, HALF), BF16),
            VMEM((4096, HALF), BF16),
            VMEM((2, HALF, CH), BF16),
            VMEM((TEMB, 2 * CH), BF16),
            VMEM((9 * CH, HALF), BF16),
            VMEM((2, TOK, CH), BF16),
            VMEM((2, 2, 8, HALF), F32),
            VMEM((EXT, CH), BF16),
            VMEM((2, EXT, HALF), BF16),
            VMEM((2, EXT, HALF), BF16),
            VMEM((2, EXT, HALF), F32),
            VMEM((3, EXT, CH), BF16),
            VMEM((3, EXT, HALF), BF16),
            VMEM((PIX, HALF), BF16),
            VMEM((PIX, HALF), BF16),
            VMEM((PIX, HALF), F32),
            VMEM((PIX, HALF), BF16),
            VMEM((PIX, HALF), BF16),
            VMEM((2, 4608, STEP), F32),
            VMEM((4608, STEP), BF16),
            VMEM((4608, STEP), BF16),
            VMEM((2, 3, 576, STEP), BF16),
            VMEM((2, 3, 576, STEP), BF16),
            VMEM((2, 576, STEP), F32),
            VMEM((2, 3, 144, STEP), BF16),
            VMEM((2, 3, 144, STEP), BF16),
            VMEM((2, 144, STEP), F32),
            VMEM((7, 48, STEP), BF16),
            VMEM((7, 48, STEP), BF16),
            VMEM((2, 512, STEP), F32),
            VMEM((512, STEP), BF16),
            VMEM((512, STEP), BF16),
            VMEM((3, 128, STEP), BF16),
            VMEM((3, 128, STEP), BF16),
            VMEM((128, STEP), F32),
            VMEM((3, 32, STEP), BF16),
            VMEM((3, 32, STEP), BF16),
            VMEM((32, STEP), F32),
            VMEM((3, 8, STEP), F32),
            VMEM((3, 8, STEP), F32),
            VMEM((8, STEP), F32),
            VMEM((2, 8, STEP), F32),
            pltpu.SemaphoreType.DMA((10,)),
            pltpu.SemaphoreType.DMA((COPIES,)),
            pltpu.SemaphoreType.DMA((COPIES,)),
        ],
        compiler_params=pltpu.CompilerParams(
            collective_id=0, has_side_effects=True, vmem_limit_bytes=60 * 1024 * 1024
        ),
        name="block",
    )(
        lengths,
        pixels.reshape(PIX, CH),
        hidden.reshape(TOK, CH),
        enc_gain.reshape(32, STEP),
        attn_gain.reshape(4, STEP),
        time_row,
        w_query,
        w_key,
        w_value,
        w_out,
        w_time,
        w_conv,
        cotangent.reshape(PIX, HALF),
    )
    result, grad_conv, grad_out_t = pl.pallas_call(
        output_kernel,
        out_shape=(
            jax.ShapeDtypeStruct((PIX, HALF), BF16),
            jax.ShapeDtypeStruct((36, HALF), F32),
            jax.ShapeDtypeStruct((4, HALF), F32),
        ),
        in_specs=[ANY] * 3,
        out_specs=(INSIDE,) * 3,
        scratch_shapes=[pltpu.SemaphoreType.DMA((3,))],
        compiler_params=pltpu.CompilerParams(vmem_limit_bytes=60 * 1024 * 1024),
        name="outputs",
    )(result, grad_conv, grad_out_t)
    return result.reshape(1, ROWS, COLS, HALF), grad_conv, grad_out_t


def solution(mesh):
    finer = Mesh(
        mesh.devices.reshape(4, 4, 4, 2, mesh.shape["chan"]),
        ("dp_0", "dp_1", "space_0", "space_1", "chan"),
    )
    placed = (
        P(DP, SPACE, None, None),
        P(DP, None, SPACE),
        P(),
        P(DP),
        P(DP),
        P(),
        P(None, "chan"),
        P(None, "chan"),
        P(None, "chan"),
        P("chan", None),
        P(),
        P(None, "chan"),
        P(DP, SPACE, None, "chan"),
    )
    return jax.shard_map(
        shards,
        mesh=finer,
        in_specs=placed,
        out_specs=(P(DP, SPACE, None, "chan"), P(DP_SPACE, "chan"), P(DP_SPACE, "chan")),
        check_vma=False,
    )
```
